128 devices in a mesh: row: 16 (over y, z), col: 8 (over x, core).
Axes of the slice: x: 4, y: 4, z: 4, core: 2. Of those that a mesh axis runs over, the one named last changes fastest.
Arguments:
- rhs: float32 [2, 16, 64, 512], P(None, 'row'), may hold values from -6 to 6
- inverse_t: float32 [2, 16, 512, 512], P(None, 'row', None, 'col'), may hold values from -1 to 2, as said below
- u_factors: bfloat16 [2, 16, 4, 8, 32, 512], P(None, 'row', None, 'col'), may hold values from -0.14941406 to 0.14941406
- v_factors: bfloat16 [2, 16, 4, 8, 32, 512], P(None, 'row', None, 'col'), may hold values from -0.14941406 to 0.14941406
- tile_ranks: int32 [2, 16, 4, 8], P(None, 'row', None, 'col'), may hold values from 8 to 32
Outputs:
- solved: float32 [2, 16, 64, 512], P(None, 'row')
The draws below stay inside these ranges and needn't reach their ends.
Inputs may be any that keep to these rules, and one draw needn't show every extreme that they name: `inverse_t`: each transposed inverse is nonsingular and of order one.
All inputs are finite; a program needn't handle non-finite values.
Results may differ from the reference program's by a relative error of at most 0.004.
Values may be sent and summed in bfloat16 or wider, within the bound.
A program may use at most 64 MiB of HBM per device.

```python
import jax
import jax.numpy as jnp
from jax import lax

B = 512
R = 64
K = 32
BR = 2
NB = 32
BC = 4
N_ROW = 16
N_COL = 8


def draw_inverse_t(key, part):
    shape = (BR, NB // BR, B, B)
    eye = jnp.eye(B, dtype=jnp.float32)
    noise = jax.random.normal(key, shape, jnp.float32) * (0.5 / B ** 0.5)
    return jnp.clip(eye + noise, -1.0, 2.0)


def plant(result, key, smallest, largest):
    spot = [jax.random.randint(jax.random.fold_in(key, axis), (), 0, length) for axis, length in enumerate(result.shape)]
    longest = result.shape.index(max(result.shape))
    next_to = spot[:longest] + [(spot[longest] + 1) % result.shape[longest]] + spot[longest + 1:]
    return result.at[tuple(spot)].set(smallest).at[tuple(next_to)].set(largest)


def shard_levels(own_key, extent, cuts, low, top_value):
    def one(dim, blocks):
        steps = jax.random.uniform(jax.random.fold_in(jax.random.fold_in(own_key, 6), dim), (blocks,), jnp.float32, low / len(cuts), top_value / len(cuts))
        return jnp.repeat(jnp.exp(steps), extent[dim] // blocks).reshape((-1,) + (1,) * (len(extent) - dim - 1))

    loudness = one(*cuts[0])
    for cut in cuts[1:]:
        loudness = loudness * one(*cut)
    return loudness


def normal_values(own_key, extent, scale, limit, cuts=(), kind=jnp.bfloat16):
    values = scale * jax.random.normal(own_key, extent, jnp.float32)
    if cuts:
        values = values * shard_levels(own_key, extent, cuts, -0.22, 0.18)
    return jnp.clip(values, -limit, limit).astype(kind)


def setup_inputs(seed: int = 0) -> dict:
    seeds = jax.random.split(jax.random.key(seed), 6)
    rhs = normal_values(seeds[0], (BR, N_ROW, R, B), 1.0, 6.0, ((1, 16),), jnp.float32)
    inverse_t = draw_inverse_t(jax.random.fold_in(seeds[5], 71), 0)
    u_factors = normal_values(seeds[2], (BR, N_ROW, BC, N_COL, K, B), 0.025, 0.14941406, ((1, 16), (3, 8)))
    v_factors = normal_values(seeds[3], (BR, N_ROW, BC, N_COL, K, B), 0.025, 0.14941406, ((1, 16), (3, 8)))
    tile_ranks = plant(jax.random.randint(seeds[4], (BR, N_ROW, BC, N_COL), K // 4, K + 1), jax.random.fold_in(seeds[4], 1), K // 4, K).astype(jnp.int32)
    return dict(rhs=rhs, inverse_t=inverse_t, u_factors=u_factors, v_factors=v_factors, tile_ranks=tile_ranks)


def pick(array, index, axis):
    return lax.dynamic_index_in_dim(array, index, axis, keepdims=False)


def reference(rhs, inverse_t, u_factors, v_factors, tile_ranks):
    blocks = BR * N_ROW
    global_rows = (jnp.arange(BR, dtype=jnp.int32)[:, None] * N_ROW + jnp.arange(N_ROW, dtype=jnp.int32)[None, :])
    rank_cols = jnp.arange(K, dtype=jnp.int32)

    def step(k, carry):
        totals, solved = carry
        k = jnp.asarray(k).astype(jnp.int32)
        k_slot = (k // N_ROW).astype(jnp.int32)
        k_row = (k % N_ROW).astype(jnp.int32)
        c_slot = (k // N_COL).astype(jnp.int32)
        c_dev = (k % N_COL).astype(jnp.int32)
        segment = pick(pick(rhs, k_slot, 0), k_row, 0) - pick(pick(totals, k_slot, 0), k_row, 0)
        inv_block = pick(pick(inverse_t, k_slot, 0), k_row, 0)
        value = jnp.dot(segment, inv_block, precision=lax.Precision.HIGHEST, preferred_element_type=jnp.float32)
        row_block = pick(solved, k_slot, 0)
        row_block = lax.dynamic_update_index_in_dim(row_block, value, k_row, 0)
        solved = lax.dynamic_update_index_in_dim(solved, row_block, k_slot, 0)
        seg_b = value.astype(jnp.bfloat16).astype(jnp.float32)
        v_col = pick(pick(v_factors, c_slot, 2), c_dev, 2).astype(jnp.float32)
        u_col = pick(pick(u_factors, c_slot, 2), c_dev, 2).astype(jnp.float32)
        ranks = pick(pick(tile_ranks, c_slot, 2), c_dev, 2)
        proj = jnp.einsum("rb,xykb->xyrk", seg_b, v_col)
        keep = (rank_cols[None, None, None, :] < ranks[:, :, None, None]) & (global_rows > k)[:, :, None, None]
        proj_b = jnp.where(keep, proj, 0.0).astype(jnp.bfloat16).astype(jnp.float32)
        update = jnp.einsum("xyrk,xykb->xyrb", proj_b, u_col)
        return totals + update, solved

    start = jnp.zeros(rhs.shape, jnp.float32)
    totals, solved = lax.fori_loop(0, blocks, step, (start, start))
    return solved
```

```python
import jax
import jax.numpy as jnp
from jax import lax
from jax.experimental import pallas as pl
from jax.experimental.pallas import tpu as pltpu
from jax.sharding import PartitionSpec as P

B = 512
R = 64
K = 32
BC = 4
N_ROW = 16
N_COL = 8
S = 16
W = 4 * K
CH = 4
F32 = jnp.float32
BF16 = jnp.bfloat16
MESH = pl.DeviceIdType.MESH


def nn(a, b):
    return jnp.dot(a, b, preferred_element_type=F32)


def nt(a, b):
    return lax.dot_general(a, b, (((1,), (1,)), ((), ())), preferred_element_type=F32)


def chain_place(m):
    row = ((m // 2) % 4) * 4 + 1 + m % 2
    col = (m // 8) * 2 + 1
    return row, col


def kernel(
    ranks, rhs, inv, u, v, out,
    um, invt, zp, zpb, zf,
    inv_all, u_all, v_all, z_all, w2, m2, acc, csum, p_in, p_out, c_out, c_in, pair_p,
    inv_s, u_s, v_s, zb_s, zf_s, p_s, c_s,
    inv_r, u_r, v_r, zb_r, zf_r, p_r, c_r,
):
    r = lax.axis_index("row")
    q = lax.axis_index("col")
    half = r // 2
    i2 = r % 2
    q2 = q % 2

    def is_me(row, col):
        return (row == r) & (col == q)

    def remote(src, dst, ssem, rsem, row, col):
        return pltpu.make_async_remote_copy(
            src_ref=src, dst_ref=dst, send_sem=ssem, recv_sem=rsem,
            device_id=(row, col), device_id_type=MESH,
        )

    def send(src, dst, ssem, rsem, row, col):
        me = is_me(row, col)

        @pl.when(me)
        def _():
            pltpu.make_async_copy(src, dst, rsem).start()

        @pl.when(jnp.logical_not(me))
        def _():
            remote(src, dst, ssem, rsem, row, col).start()

    def sent(src, dst, ssem, rsem, row, col):
        @pl.when(jnp.logical_not(is_me(row, col)))
        def _():
            remote(src, dst, ssem, rsem, row, col).wait_send()

    def arrived(dst, rsem):
        pltpu.make_async_copy(dst, dst, rsem).wait()

    def inv_copy(a):
        return (
            invt.at[pl.ds(a * R, R)], inv_all.at[i2, pl.ds(pl.multiple_of(q * R, R), R)],
            inv_s.at[a], inv_r.at[i2, q], *chain_place(8 * a + half),
        )

    def u_copy(a, c):
        return (
            um.at[a, c], u_all.at[4 * c + q // 2, pl.ds(pl.multiple_of((q2 * 2 + i2) * K, K), K)],
            u_s.at[a, c], u_r.at[i2, 8 * c + q], *chain_place(8 * a + half),
        )

    def v_copy(a, c):
        return (
            v.at[a, c], v_all.at[8 * a + half, pl.ds(pl.multiple_of((q2 * 2 + i2) * K, K), K)],
            v_s.at[a, c], v_r.at[q2, 16 * a + r], *chain_place(4 * c + q // 2),
        )

    def below(a, c):
        return 8 * c + q < 16 * a + r

    def zb_copy(a):
        return (zpb, z_all.at[i2, q], zb_s.at[a], zb_r.at[i2, q], *chain_place(8 * a + half))

    def zf_copy(step):
        return (zp, zf.at[q], zf_s.at[step], zf_r.at[q], r, (q + step) % N_COL)

    for c in range(BC):
        for a in range(2):
            @pl.when(below(a, c))
            def _(a=a, c=c):
                send(*v_copy(a, c))

    both = jnp.concatenate([inv[0], inv[1]], axis=1)
    invt[...] = both.T.astype(BF16)
    for a in range(2):
        send(*inv_copy(a))

    rank_rows = lax.broadcasted_iota(jnp.int32, (K, B), 0)
    for a in range(2):
        for c in range(BC):
            um[a, c] = jnp.where(rank_rows < ranks[a, c], u[a, c].astype(F32), 0.0).astype(BF16)

            @pl.when(below(a, c))
            def _(a=a, c=c):
                send(*u_copy(a, c))

    z_mine = [
        jnp.dot(rhs[a], inv[a], precision=lax.Precision.HIGHEST, preferred_element_type=F32)
        for a in range(2)
    ]
    packed = jnp.concatenate(z_mine, axis=1)
    zp[...] = packed
    zpb[...] = packed.astype(BF16)
    for a in range(2):
        send(*zb_copy(a))
    for step in range(N_COL):
        send(*zf_copy(step))

    z_level = (r % 4) - 1
    m = (q // 2) * 8 + (r // 4) * 2 + z_level
    chains = (q2 == 1) & (q < 4) & ((z_level == 0) | (z_level == 1))

    def c_copy(b2, col):
        line = (2 * m + b2) % N_ROW
        return (c_out.at[b2], c_in.at[m // 8], c_s.at[b2, col], c_r.at[m // 8], line, col)

    def p_copy(t):
        return (p_out.at[t], p_in.at[m], p_s.at[t], p_r.at[m], *chain_place(t))

    @pl.when(chains)
    def _():
        lanes = lax.broadcasted_iota(jnp.int32, (1, CH * W), 1) % W < W // 2
        rows = lax.broadcasted_iota(jnp.int32, (W, 1), 0) % (2 * K) < K
        first = (m + 1) // CH

        for b2 in range(2):
            for col in range(N_COL):
                arrived(inv_all.at[b2, pl.ds(col * R, R)], inv_r.at[b2, col])
                arrived(z_all.at[b2, col], zb_r.at[b2, col])

            @pl.loop(0, 2 * m + b2)
            def _(l, b2=b2):
                arrived(u_all.at[l // 2, pl.ds(pl.multiple_of((l % 2) * 2 * K + b2 * K, K), K)], u_r.at[b2, l])

            @pl.loop(2 * m + b2 + 1, 2 * S)
            def _(i, b2=b2):
                arrived(v_all.at[i // 2, pl.ds(pl.multiple_of(b2 * 2 * K + (i % 2) * K, K), K)], v_r.at[b2, i])

        slot = m // 8

        def slices(b2, a):
            return jnp.concatenate([z_all[b2, col][:, a * R:(a + 1) * R] for col in range(N_COL)], axis=1)

        def joined(b2):
            return jnp.where(slot == 0, slices(b2, 0).astype(F32), slices(b2, 1).astype(F32))

        v10 = v_all[m, K:2 * K]
        w10 = nn(u_all[m, K:2 * K], jnp.transpose(inv_all[1].astype(F32)).astype(BF16)).astype(BF16)
        z0 = joined(0).astype(BF16)
        inner = nn(nt(z0, v10).astype(BF16), w10)
        z1 = (joined(1) - inner).astype(BF16)
        csum[:, :B] = jnp.zeros((R, B), F32)
        csum[:, B:] = inner
        pair_p[:, :B] = z0
        pair_p[:, B:] = z1

        @pl.loop(0, m)
        def _(lb):
            ub = u_all[lb]
            wa = jnp.where(rows, nt(ub, inv_all[0]), 0.0).astype(BF16)
            mixed = nn(nt(wa, v10).astype(BF16), w10)
            wb = (jnp.where(rows, 0.0, nt(ub, inv_all[1])) - mixed).astype(BF16)
            w2[lb, :, :B] = wa
            w2[lb, :, B:] = wb

            @pl.loop(first, S // CH)
            def _(ch):
                vc = v_all[pl.ds(ch * CH, CH)].reshape(CH * W, B)
                m2[lb, ch] = jnp.where(lanes, nt(wa, vc), nt(wb, vc)).astype(BF16)

        @pl.loop(first, S // CH)
        def _(ch):
            vc = v_all[pl.ds(ch * CH, CH)].reshape(CH * W, B)
            acc[ch] = jnp.where(lanes, nt(pair_p[:, :B], vc), nt(pair_p[:, B:], vc))

        @pl.loop(0, m - 1)
        def _(lb):
            arrived(p_in.at[lb], p_r.at[lb])
            p = p_in[lb]

            @pl.loop(first, S // CH)
            def _(ch):
                acc[ch] = acc[ch] - nn(p, m2[lb, ch])

            csum[...] = csum[...] + nn(p, w2[lb])

        last = jnp.maximum(m - 1, 0)

        @pl.when(m > 0)
        def _():
            arrived(p_in.at[last], p_r.at[last])

            @pl.loop(m + 1, S)
            def _(t):
                cols = pl.ds(pl.multiple_of((t % CH) * W, W), W)
                block = acc[t // CH, :, cols] - nn(p_in[last], m2[last, t // CH, :, cols])
                p_out[t] = block.astype(BF16)
                remote(*p_copy(t)).start()

            csum[...] = csum[...] + nn(p_in[last], w2[last])

        @pl.when(m == 0)
        def _():
            @pl.loop(1, S)
            def _(t):
                cols = pl.ds(pl.multiple_of((t % CH) * W, W), W)
                p_out[t] = acc[t // CH, :, cols].astype(BF16)
                remote(*p_copy(t)).start()

        for b2 in range(2):
            c_out[b2] = csum[:, b2 * B:(b2 + 1) * B].astype(BF16)

            @pl.loop(0, N_COL)
            def _(col, b2=b2):
                send(*c_copy(b2, col))

    for col in range(N_COL):
        arrived(zf.at[col], zf_r.at[col])
    for a in range(2):
        z = jnp.concatenate([zf[col][:, a * R:(a + 1) * R] for col in range(N_COL)], axis=1)
        arrived(c_in.at[a], c_r.at[a])
        out[a] = z - c_in[a].astype(F32)

    for a in range(2):
        sent(*inv_copy(a))
        sent(*zb_copy(a))
        for c in range(BC):
            @pl.when(below(a, c))
            def _(a=a, c=c):
                sent(*u_copy(a, c))
                sent(*v_copy(a, c))
    for step in range(1, N_COL):
        sent(*zf_copy(step))

    @pl.when(chains)
    def _():
        @pl.loop(m + 1, S)
        def _(t):
            remote(*p_copy(t)).wait_send()

        for b2 in range(2):
            @pl.loop(0, N_COL)
            def _(col, b2=b2):
                sent(*c_copy(b2, col))


def on_device(rhs, inverse_t, u_factors, v_factors, tile_ranks):
    vmem = pl.BlockSpec(memory_space=pltpu.VMEM)
    dma = pltpu.SemaphoreType.DMA
    solved = pl.pallas_call(
        kernel,
        out_shape=jax.ShapeDtypeStruct((2, R, B), F32),
        in_specs=[pl.BlockSpec(memory_space=pltpu.SMEM), vmem, vmem, vmem, vmem],
        out_specs=vmem,
        scratch_shapes=[
            pltpu.VMEM((2, BC, K, B), BF16),
            pltpu.VMEM((2 * R, B), BF16),
            pltpu.VMEM((R, 2 * R), F32),
            pltpu.VMEM((R, 2 * R), BF16),
            pltpu.VMEM((N_COL, R, 2 * R), F32),
            pltpu.VMEM((2, B, B), BF16),
            pltpu.VMEM((S, W, B), BF16),
            pltpu.VMEM((S, W, B), BF16),
            pltpu.VMEM((2, N_COL, R, 2 * R), BF16),
            pltpu.VMEM((S, W, 2 * B), BF16),
            pltpu.VMEM((S, S // CH, W, CH * W), BF16),
            pltpu.VMEM((S // CH, R, CH * W), F32),
            pltpu.VMEM((R, 2 * B), F32),
            pltpu.VMEM((S, R, W), BF16),
            pltpu.VMEM((S, R, W), BF16),
            pltpu.VMEM((2, R, B), BF16),
            pltpu.VMEM((2, R, B), BF16),
            pltpu.VMEM((R, 2 * B), BF16),
            dma((2,)), dma((2, BC)), dma((2, BC)), dma((2,)), dma((N_COL,)), dma((S,)), dma((2, N_COL)),
            dma((2, N_COL)), dma((2, 2 * S)), dma((2, 2 * S)), dma((2, N_COL)), dma((N_COL,)), dma((S,)), dma((2,)),
        ],
        compiler_params=pltpu.CompilerParams(has_side_effects=True),
    )(
        tile_ranks[:, 0, :, 0], rhs[:, 0], inverse_t[:, 0], u_factors[:, 0, :, 0], v_factors[:, 0, :, 0]
    )
    return solved[:, None]


def solution(mesh):
    in_specs = (
        P(None, "row", None, None),
        P(None, "row", None, "col"),
        P(None, "row", None, "col", None, None),
        P(None, "row", None, "col", None, None),
        P(None, "row", None, "col"),
    )
    out_specs = P(None, "row", None, None)
    return jax.shard_map(
        on_device, mesh=mesh, in_specs=in_specs, out_specs=out_specs, check_vma=False
    )
```

```python
import jax
import jax.numpy as jnp
from jax import lax
from jax.experimental import pallas as pl
from jax.experimental.pallas import tpu as pltpu
from jax.sharding import PartitionSpec as P

B = 512
R = 64
K = 32
BC = 4
N_ROW = 16
N_COL = 8
NB = 32
T = 4
NG = NB // T
L = T * K
WIDE = L * (NG + 1)
F32 = jnp.float32
BF16 = jnp.bfloat16
MESH = pl.DeviceIdType.MESH


def nn(a, b):
    return jnp.dot(a, b, preferred_element_type=F32)


def nt(a, b, precision=None):
    return lax.dot_general(a, b, (((1,), (1,)), ((), ())), precision=precision, preferred_element_type=F32)


def row_place(j):
    x = ((j % 8) // 2 + 2 * (j // N_ROW)) % 4
    return j % N_ROW, 2 * x + 1


def chain_place(g):
    late = g // 4
    return (g % 4) * 4 + 1 + late, 2 * (1 + late) + 1


def lane_slice(g, count=1):
    return pl.ds(pl.multiple_of(g * L, L), count * L)


def kernel(
    ranks, rhs, inv, u, v, out,
    um, invt, zp, zpb, zf,
    inv_all, u_all, v_all, z_all, w, m_out, g_out, p_row, c_out, c_in,
    m_in, m_own, acc, p_in, p_out, slab,
    inv_s, u_s, v_s, zb_s, zf_s, m_s, own_s, g_s, pc_s, pr_s, c_s,
    inv_r, u_r, v_r, zb_r, zf_r, m_r, own_r, g_r, pc_r, pr_r, c_r,
):
    r = lax.axis_index("row")
    q = lax.axis_index("col")

    q_odd = q % 2 == 1
    x_here = q // 2
    late_row = jnp.where((x_here - (r % 8) // 2) % 4 == 2, 1, 0)
    j_here = r + N_ROW * late_row
    is_row = q_odd & ((x_here - (r % 8) // 2) % 2 == 0)
    g_row = j_here // T
    t_row = j_here % T
    late_chain = jnp.where(r % 4 == 2, 1, 0)
    g_here = r // 4 + 4 * late_chain
    is_chain = q_odd & (x_here == 1 + late_chain) & (r % 4 == 1 + late_chain)

    def is_me(row, col):
        return (row == r) & (col == q)

    def remote(src, dst, ssem, rsem, row, col):
        return pltpu.make_async_remote_copy(
            src_ref=src, dst_ref=dst, send_sem=ssem, recv_sem=rsem,
            device_id=(row, col), device_id_type=MESH,
        )

    def send(src, dst, ssem, rsem, row, col):
        me = is_me(row, col)

        @pl.when(me)
        def _():
            pltpu.make_async_copy(src, dst, rsem).start()

        @pl.when(jnp.logical_not(me))
        def _():
            remote(src, dst, ssem, rsem, row, col).start()

    def sent(src, dst, ssem, rsem, row, col):
        @pl.when(jnp.logical_not(is_me(row, col)))
        def _():
            remote(src, dst, ssem, rsem, row, col).wait_send()

    def arrived(dst, rsem):
        pltpu.make_async_copy(dst, dst, rsem).wait()

    barrier = pltpu.get_barrier_semaphore()

    def greet(row, col):
        @pl.when(jnp.logical_not(is_me(row, col)))
        def _():
            pl.semaphore_signal(barrier, inc=1, device_id=(row, col), device_id_type=MESH)

    for step in range(1, N_COL):
        greet(r, (q + step) % N_COL)

    @pl.when(is_row)
    def _():
        @pl.loop(0, N_ROW)
        def _(row):
            greet(row, j_here % N_COL)

        @pl.loop(0, g_row + 1)
        def _(g):
            greet(*chain_place(g))

    @pl.when(is_chain)
    def _():
        for t in range(T):
            greet(*row_place(g_here * T + t))

        @pl.loop(0, g_here)
        def _(g):
            greet(*chain_place(g))

    expected = N_COL - 1
    for c in range(BC):
        expected += jnp.where(is_me(*row_place(8 * c + q)), 0, 1)
    expected += jnp.where(is_row, 1, 0)
    expected += jnp.where(is_chain, (NG - 1 - g_here) + T * (NG - g_here), 0)

    def inv_copy(a):
        return (
            invt.at[a], inv_all.at[pl.ds(pl.multiple_of(q * R, R), R)],
            inv_s.at[a], inv_r.at[q], *row_place(N_ROW * a + r),
        )

    def u_copy(a, c):
        return (um.at[a, c], u_all.at[8 * c + q], u_s.at[a, c], u_r.at[8 * c + q], *row_place(N_ROW * a + r))

    def v_copy(a, c):
        return (v.at[a, c], v_all.at[N_ROW * a + r], v_s.at[a, c], v_r.at[N_ROW * a + r], *row_place(8 * c + q))

    def below(a, c):
        return 8 * c + q < N_ROW * a + r

    def zb_copy(a):
        return (zpb.at[a], z_all.at[q], zb_s.at[a], zb_r.at[q], *row_place(N_ROW * a + r))

    def zf_copy(step):
        return (zp, zf.at[q], zf_s.at[step], zf_r.at[q], r, (q + step) % N_COL)

    invt[...] = inv[...].astype(BF16)
    rank_rows = lax.broadcasted_iota(jnp.int32, (K, B), 0)
    for a in range(2):
        for c in range(BC):
            um[a, c] = jnp.where(rank_rows < ranks[a, c], u[a, c].astype(F32), 0.0).astype(BF16)

    pl.semaphore_wait(barrier, expected)

    for c in range(BC):
        for a in range(2):
            @pl.when(below(a, c))
            def _(a=a, c=c):
                send(*v_copy(a, c))
    for a in range(2):
        send(*inv_copy(a))
    for a in range(2):
        for c in range(BC):
            @pl.when(below(a, c))
            def _(a=a, c=c):
                send(*u_copy(a, c))

    z_mine = [nt(rhs[a], inv[a], lax.Precision.HIGHEST) for a in range(2)]
    packed = jnp.concatenate(z_mine, axis=1)
    zp[...] = packed
    for a in range(2):
        wide = jnp.concatenate([z_mine[a], z_mine[a]], axis=1)
        keep = lax.broadcasted_iota(jnp.int32, (R, 2 * R), 1) // R == q % 2
        zpb[a] = jnp.where(keep, wide, 0.0).astype(BF16)
        send(*zb_copy(a))
    for step in range(N_COL):
        send(*zf_copy(step))

    def half_lanes(k):
        return pl.ds(2 * L * k, WIDE - L - 2 * L * k)

    def m_copy(lb, k):
        return (
            m_out.at[lb, :, half_lanes(k)], m_in.at[t_row, lb, :, half_lanes(k)],
            m_s.at[lb], m_r.at[t_row, lb], *chain_place(g_row),
        )

    def own_copy(s, k):
        return (
            m_out.at[g_row, pl.ds(s * K, K), half_lanes(k)],
            m_own.at[s, t_row, pl.ds(pl.multiple_of(t_row * K, K), K), half_lanes(k)],
            own_s.at[s], own_r.at[s, t_row], *chain_place(g_row),
        )

    def g_copy(k):
        return (
            g_out.at[:, half_lanes(k)], acc.at[t_row, :, half_lanes(k)],
            g_s.at[0], g_r.at[t_row], *chain_place(g_row),
        )

    def by_width(group, do):
        for k in range(NG // 2):
            @pl.when(group // 2 == k)
            def _(k=k):
                do(k)

    def c_copy(col):
        return (c_out, c_in.at[j_here // N_ROW], c_s.at[col], c_r.at[j_here // N_ROW], r, col)

    @pl.when(is_row)
    def _():
        @pl.loop(g_row * T, j_here + 1)
        def _(i):
            v_all[i] = jnp.zeros((K, B), BF16)

        for col in range(N_COL):
            arrived(z_all.at[col], zb_r.at[col])

        @pl.loop(j_here + 1, NB)
        def _(i):
            arrived(v_all.at[i], v_r.at[i])

        z = jnp.concatenate([z_all[2 * h] + z_all[2 * h + 1] for h in range(N_COL // 2)], axis=1)

        @pl.loop(g_row // 2, NG // 2)
        def _(h):
            cols = pl.ds(pl.multiple_of(h * 2 * L, 2 * L), 2 * L)
            g_out[:, cols] = nt(z, v_all[pl.ds(h * 2 * T, 2 * T)].reshape(2 * L, B))

        by_width(g_row, lambda k: remote(*g_copy(k)).start())

        for col in range(N_COL):
            arrived(inv_all.at[pl.ds(col * R, R)], inv_r.at[col])

        rows = lax.broadcasted_iota(jnp.int32, (L, 1), 0) // K

        @pl.loop(0, g_row + 1)
        def _(lb):
            @pl.loop(0, jnp.minimum(T, j_here - lb * T))
            def _(l):
                arrived(u_all.at[lb * T + l], u_r.at[lb * T + l])

            wl = nt(u_all[pl.ds(lb * T, T)].reshape(L, B), inv_all[...])
            wl = jnp.where(rows + lb * T < j_here, wl, 0.0).astype(BF16)
            w[lb] = wl

            @pl.loop(g_row // 2, NG // 2)
            def _(h):
                cols = pl.ds(pl.multiple_of(h * 2 * L, 2 * L), 2 * L)
                m_out[lb, :, cols] = nt(wl, v_all[pl.ds(h * 2 * T, 2 * T)].reshape(2 * L, B)).astype(BF16)

            @pl.when(lb < g_row)
            def _():
                by_width(g_row, lambda k: remote(*m_copy(lb, k)).start())

            @pl.when(lb == g_row)
            def _():
                @pl.loop(0, t_row)
                def _(s):
                    by_width(g_row, lambda k: remote(*own_copy(s, k)).start())

    def p_chain_copy(g):
        return (p_out.at[g], p_in.at[g_here], pc_s.at[g], pc_r.at[g_here], *chain_place(g))

    def p_row_copy(g, i):
        return (p_out.at[g, i], p_row.at[g_here], pr_s.at[g, i], pr_r.at[g_here], *row_place(g * T + i))

    @pl.when(is_chain)
    def _():
        quarter = lax.broadcasted_iota(jnp.int32, (R, L), 1) // K
        last = jnp.maximum(g_here - 1, 0)

        def across(parts):
            gives = []
            for i in range(T):
                row = parts[0] if i == 0 else pltpu.roll(parts[0], (L - K * i) % L, 1)
                for t in range(1, T):
                    shift = (K * (t - i)) % L
                    row = jnp.where(quarter == t, parts[t] if shift == 0 else pltpu.roll(parts[t], shift, 1), row)
                gives.append(row)
            return gives

        for s in range(T):
            for t in range(s + 1, T):
                for i in range(T):
                    if i != t:
                        m_own[s, t, i * K:(i + 1) * K, :] = jnp.zeros((K, WIDE), BF16)

        @pl.when(g_here == 0)
        def _():
            p_in[0] = jnp.zeros((T, R, L), BF16)
            for t in range(T):
                m_in[t, 0] = jnp.zeros((L, WIDE), BF16)

        def wait_g(k):
            for t in range(T):
                arrived(acc.at[t, :, half_lanes(k)], g_r.at[t])

        def wait_own(k):
            for t in range(T):
                for s in range(t):
                    arrived(m_own.at[s, t, pl.ds(t * K, K), half_lanes(k)], own_r.at[s, t])

        def wait_m(lb):
            def of(k):
                for t in range(T):
                    arrived(m_in.at[t, lb, :, half_lanes(k)], m_r.at[t, lb])

            by_width(g_here, of)

        by_width(g_here, wait_g)

        @pl.loop(0, g_here - 1)
        def _(lb):
            wait_m(lb)
            arrived(p_in.at[lb], pc_r.at[lb])

            @pl.loop(g_here // 2, NG // 2)
            def _(h):
                cols = pl.ds(pl.multiple_of(h * 2 * L, 2 * L), 2 * L)
                for t in range(T):
                    acc[t, :, cols] = acc[t, :, cols] - nn(p_in[lb, t], m_in[t, lb, :, cols])

        @pl.when(g_here > 0)
        def _():
            wait_m(last)

        by_width(g_here, wait_own)

        @pl.when(g_here > 0)
        def _():
            arrived(p_in.at[last], pc_r.at[last])

        near = lane_slice(g_here, 2)
        found, inner = [], []
        for t in range(T):
            x = acc[t, :, near] - nn(p_in[last, t], m_in[t, last, :, near])
            for s in range(t):
                x = x - nn(inner[s], m_own[s, t, :, near])
            found.append(x)
            inner.append(x[:, :L].astype(BF16))

        @pl.when(g_here < NG - 1)
        def _():
            for i, block in enumerate(across([x[:, L:] for x in found])):
                p_out[g_here + 1, i] = block.astype(BF16)
            remote(*p_chain_copy(g_here + 1)).start()

        for i, block in enumerate(across([x[:, :L] for x in found])):
            p_out[g_here, i] = jnp.where(quarter < i, block, 0.0).astype(BF16)
            remote(*p_row_copy(g_here, i)).start()

        @pl.when(g_here < NG - 1)
        def _():
            for i in range(T):
                remote(*p_row_copy(g_here + 1, i)).start()
            for t in range(T):
                slab[t] = inner[t]

        @pl.loop(g_here + 2, NG)
        def _(g):
            cols = lane_slice(g)
            far = []
            for t in range(T):
                x = acc[t, :, cols] - nn(p_in[last, t], m_in[t, last, :, cols])
                for s in range(t):
                    x = x - nn(slab[s], m_own[s, t, :, cols])
                far.append(x)
            for i, block in enumerate(across(far)):
                p_out[g, i] = block.astype(BF16)
            remote(*p_chain_copy(g)).start()
            for i in range(T):
                remote(*p_row_copy(g, i)).start()

    @pl.when(is_row)
    def _():
        def term(g):
            arrived(p_row.at[g], pr_r.at[g])
            return nn(p_row[g], w[g])

        correction = lax.fori_loop(0, g_row + 1, lambda g, total: total + term(g), jnp.zeros((R, B), F32))
        c_out[...] = correction.astype(BF16)
        for col in range(N_COL):
            send(*c_copy(col))

    for col in range(N_COL):
        arrived(zf.at[col], zf_r.at[col])
    for a in range(2):
        z = jnp.concatenate([zf[col][:, a * R:(a + 1) * R] for col in range(N_COL)], axis=1)
        arrived(c_in.at[a], c_r.at[a])
        out[a] = z - c_in[a].astype(F32)

    for a in range(2):
        sent(*inv_copy(a))
        sent(*zb_copy(a))
        for c in range(BC):
            @pl.when(below(a, c))
            def _(a=a, c=c):
                sent(*u_copy(a, c))
                sent(*v_copy(a, c))
    for step in range(1, N_COL):
        sent(*zf_copy(step))

    @pl.when(is_row)
    def _():
        by_width(g_row, lambda k: remote(*g_copy(k)).wait_send())

        @pl.loop(0, g_row)
        def _(lb):
            by_width(g_row, lambda k: remote(*m_copy(lb, k)).wait_send())

        @pl.loop(0, t_row)
        def _(s):
            by_width(g_row, lambda k: remote(*own_copy(s, k)).wait_send())

        for col in range(N_COL):
            sent(*c_copy(col))

    @pl.when(is_chain)
    def _():
        @pl.loop(g_here, NG)
        def _(g):
            for i in range(T):
                remote(*p_row_copy(g, i)).wait_send()

        @pl.loop(g_here + 1, NG)
        def _(g):
            remote(*p_chain_copy(g)).wait_send()


def on_device(rhs, inverse_t, u_factors, v_factors, tile_ranks):
    vmem = pl.BlockSpec(memory_space=pltpu.VMEM)
    dma = pltpu.SemaphoreType.DMA
    solved = pl.pallas_call(
        kernel,
        out_shape=jax.ShapeDtypeStruct((2, R, B), F32),
        in_specs=[pl.BlockSpec(memory_space=pltpu.SMEM), vmem, vmem, vmem, vmem],
        out_specs=vmem,
        scratch_shapes=[
            pltpu.VMEM((2, BC, K, B), BF16),
            pltpu.VMEM((2, R, B), BF16),
            pltpu.VMEM((R, 2 * R), F32),
            pltpu.VMEM((2, R, 2 * R), BF16),
            pltpu.VMEM((N_COL, R, 2 * R), F32),
            pltpu.VMEM((B, B), BF16),
            pltpu.VMEM((NB, K, B), BF16),
            pltpu.VMEM((NB, K, B), BF16),
            pltpu.VMEM((N_COL, R, 2 * R), BF16),
            pltpu.VMEM((NG, L, B), BF16),
            pltpu.VMEM((NG, L, WIDE), BF16),
            pltpu.VMEM((R, WIDE), F32),
            pltpu.VMEM((NG, R, L), BF16),
            pltpu.VMEM((R, B), BF16),
            pltpu.VMEM((2, R, B), BF16),
            pltpu.VMEM((T, NG, L, WIDE), BF16),
            pltpu.VMEM((T, T, L, WIDE), BF16),
            pltpu.VMEM((T, R, WIDE), F32),
            pltpu.VMEM((NG, T, R, L), BF16),
            pltpu.VMEM((NG, T, R, L), BF16),
            pltpu.VMEM((T, R, L), BF16),
            dma((2,)), dma((2, BC)), dma((2, BC)), dma((2,)), dma((N_COL,)),
            dma((NG,)), dma((T,)), dma((1,)), dma((NG,)), dma((NG, T)), dma((N_COL,)),
            dma((N_COL,)), dma((NB,)), dma((NB,)), dma((N_COL,)), dma((N_COL,)),
            dma((T, NG)), dma((T, T)), dma((T,)), dma((NG,)), dma((NG,)), dma((2,)),
        ],
        compiler_params=pltpu.CompilerParams(has_side_effects=True, collective_id=0),
    )(
        tile_ranks[:, 0, :, 0], rhs[:, 0], jnp.swapaxes(inverse_t[:, 0], 1, 2),
        u_factors[:, 0, :, 0], v_factors[:, 0, :, 0],
    )
    return solved[:, None]


def solution(mesh):
    in_specs = (
        P(None, "row", None, None),
        P(None, "row", None, "col"),
        P(None, "row", None, "col", None, None),
        P(None, "row", None, "col", None, None),
        P(None, "row", None, "col"),
    )
    out_specs = P(None, "row", None, None)
    return jax.shard_map(
        on_device, mesh=mesh, in_specs=in_specs, out_specs=out_specs, check_vma=False
    )
```

```python
import jax
import jax.numpy as jnp
from jax import lax
from jax.experimental import pallas as pl
from jax.experimental.pallas import tpu as pltpu
from jax.sharding import PartitionSpec as P

B = 512
R = 64
K = 32
BC = 4
N_ROW = 16
N_COL = 8
NB = 32
T = 4
NG = NB // T
L = T * K
NEAR = 3
WIDE = L * (NG + 2)
F32 = jnp.float32
BF16 = jnp.bfloat16
MESH = pl.DeviceIdType.MESH


def nn(a, b):
    return jnp.dot(a, b, preferred_element_type=F32)


def nt(a, b, precision=None):
    return lax.dot_general(a, b, (((1,), (1,)), ((), ())), precision=precision, preferred_element_type=F32)


def row_place(j):
    x = ((j % 8) // 2 + 2 * (j // N_ROW)) % 4
    return j % N_ROW, 2 * x + 1


def chain_place(g):
    late = g // 4
    return (g % 4) * 4 + 1 + late, 2 * (1 + late) + 1


def kernel(
    ranks, rhs_hbm, inv_hbm, u_hbm, v_hbm, out,
    rhs, inv, u, v, um, invt, zp, zpb, zf,
    inv_all, u_all, v_all, z_all, w, m_out, g_out, p_row, s_out, c_out, c_in,
    m_in, m_own, acc, s_in, p_in, p_out,
    in_s, inv_s, u_s, v_s, zb_s, zf_s, m_s, own_s, g_s, s_s, pc_s, pr_s, relay_s, c_s,
    inv_r, u_r, v_r, zb_r, zf_r, m_r, own_r, g_r, s_r, pc_r, pr_r, c_r,
):
    r = lax.axis_index("row")
    q = lax.axis_index("col")

    q_odd = q % 2 == 1
    x_here = q // 2
    late_row = jnp.where((x_here - (r % 8) // 2) % 4 == 2, 1, 0)
    j_here = r + N_ROW * late_row
    is_row = q_odd & ((x_here - (r % 8) // 2) % 2 == 0)
    g_row = j_here // T
    t_row = j_here % T
    late_chain = jnp.where(r % 4 == 2, 1, 0)
    g_here = r // 4 + 4 * late_chain
    is_chain = q_odd & (x_here == 1 + late_chain) & (r % 4 == 1 + late_chain)

    def is_me(row, col):
        return (row == r) & (col == q)

    def remote(src, dst, ssem, rsem, row, col):
        return pltpu.make_async_remote_copy(
            src_ref=src, dst_ref=dst, send_sem=ssem, recv_sem=rsem,
            device_id=(row, col), device_id_type=MESH,
        )

    def send(src, dst, ssem, rsem, row, col):
        me = is_me(row, col)

        @pl.when(me)
        def _():
            pltpu.make_async_copy(src, dst, rsem).start()

        @pl.when(jnp.logical_not(me))
        def _():
            remote(src, dst, ssem, rsem, row, col).start()

    def sent(src, dst, ssem, rsem, row, col):
        @pl.when(jnp.logical_not(is_me(row, col)))
        def _():
            remote(src, dst, ssem, rsem, row, col).wait_send()

    def arrived(dst, rsem):
        pltpu.make_async_copy(dst, dst, rsem).wait()

    barrier = pltpu.get_barrier_semaphore()

    def greet(row, col):
        @pl.when(jnp.logical_not(is_me(row, col)))
        def _():
            pl.semaphore_signal(barrier, inc=1, device_id=(row, col), device_id_type=MESH)

    for step in range(1, N_COL):
        greet(r, (q + step) % N_COL)

    @pl.when(is_row)
    def _():
        @pl.loop(0, N_ROW)
        def _(row):
            greet(row, j_here % N_COL)

        @pl.loop(jnp.maximum(g_row - NEAR + 1, 0), g_row + 1)
        def _(g):
            greet(*chain_place(g))

    @pl.when(is_chain)
    def _():
        for t in range(T):
            greet(*row_place(g_here * T + t))

        @pl.loop(jnp.maximum(g_here - NEAR + 1, 0), g_here)
        def _(g):
            greet(*chain_place(g))

        @pl.loop(0, T * (g_here - NEAR + 1))
        def _(j):
            greet(*row_place(j))

    expected = N_COL - 1
    for c in range(BC):
        expected += jnp.where(is_me(*row_place(8 * c + q)), 0, 1)
    expected += jnp.where(is_row, 1 + jnp.maximum(NG - NEAR - g_row, 0), 0)
    after = jnp.minimum(NEAR - 1, NG - 1 - g_here)
    expected += jnp.where(is_chain, after + T * (after + 1), 0)

    def inv_copy(a):
        return (
            invt.at[a], inv_all.at[pl.ds(pl.multiple_of(q * R, R), R)],
            inv_s.at[a], inv_r.at[q], *row_place(N_ROW * a + r),
        )

    def u_copy(a, c):
        return (um.at[a, c], u_all.at[8 * c + q], u_s.at[a, c], u_r.at[8 * c + q], *row_place(N_ROW * a + r))

    def v_copy(a, c):
        return (v.at[a, c], v_all.at[N_ROW * a + r], v_s.at[a, c], v_r.at[N_ROW * a + r], *row_place(8 * c + q))

    def below(a, c):
        return 8 * c + q < N_ROW * a + r

    def zb_copy(a):
        return (zpb.at[a], z_all.at[q], zb_s.at[a], zb_r.at[q], *row_place(N_ROW * a + r))

    def zf_copy(step):
        return (zp, zf.at[q], zf_s.at[step], zf_r.at[q], r, (q + step) % N_COL)

    loads = [
        pltpu.make_async_copy(src, dst, in_s.at[k])
        for k, (src, dst) in enumerate([(inv_hbm, inv), (rhs_hbm, rhs), (u_hbm, u), (v_hbm, v)])
    ]
    for load in loads:
        load.start()
    for load in loads:
        load.wait()
    invt[...] = inv[...].astype(BF16)
    rank_rows = lax.broadcasted_iota(jnp.int32, (K, B), 0)
    for a in range(2):
        for c in range(BC):
            um[a, c] = jnp.where(rank_rows < ranks[a, c], u[a, c].astype(F32), 0.0).astype(BF16)
    z_mine = [nt(rhs[a], inv[a], lax.Precision.HIGHEST) for a in range(2)]
    zp[...] = jnp.concatenate(z_mine, axis=1)
    for a in range(2):
        wide = jnp.concatenate([z_mine[a], z_mine[a]], axis=1)
        keep = lax.broadcasted_iota(jnp.int32, (R, 2 * R), 1) // R == q % 2
        zpb[a] = jnp.where(keep, wide, 0.0).astype(BF16)

    pl.semaphore_wait(barrier, expected)

    def near(a, c):
        return (N_ROW * a + r) // T - (8 * c + q) // T < NEAR

    def each_v(do, wanted, columns):
        for c in columns:
            for a in range(2):
                @pl.when(below(a, c) & (near(a, c) == wanted))
                def _(a=a, c=c):
                    do(*v_copy(a, c))

    def each_u(do, a):
        for c in range(BC):
            @pl.when(below(a, c))
            def _(c=c):
                do(*u_copy(a, c))

    def first_wave(do):
        do(*zb_copy(0))
        do(*zb_copy(1))
        each_v(do, True, (0, 1))
        do(*inv_copy(0))
        each_u(do, 0)

    def second_wave(do):
        each_v(do, True, (2, 3))
        do(*inv_copy(1))
        each_u(do, 1)

    first_wave(send)
    first_wave(sent)
    second_wave(send)
    each_v(send, False, range(BC))
    for step in range(N_COL):
        send(*zf_copy(step))

    def lanes_of(g, count):
        return pl.ds(pl.multiple_of(g * L, L), count * L)

    def m_copy(lb):
        lanes = lanes_of(g_row, NEAR)
        return (
            m_out.at[lb, :, lanes], m_in.at[t_row, lb, :, lanes],
            m_s.at[lb], m_r.at[t_row, lb], *chain_place(g_row),
        )

    def own_copy(s):
        lanes = lanes_of(g_row, NEAR)
        return (
            m_out.at[g_row, pl.ds(s * K, K), lanes],
            m_own.at[s, t_row, pl.ds(pl.multiple_of(t_row * K, K), K), lanes],
            own_s.at[s], own_r.at[s, t_row], *chain_place(g_row),
        )

    def g_copy():
        lanes = lanes_of(g_row, NEAR)
        return (
            g_out.at[:, lanes], acc.at[t_row, :, lanes],
            g_s.at[0], g_r.at[t_row], *chain_place(g_row),
        )

    def slab_copy(g):
        return (s_out.at[g], s_in.at[g_row, t_row], s_s.at[g], s_r.at[g_row, t_row], *chain_place(g))

    def c_copy(col):
        return (c_out, c_in.at[j_here // N_ROW], c_s.at[col], c_r.at[j_here // N_ROW], r, col)

    @pl.when(is_row)
    def _():
        here = lanes_of(g_row, NEAR)
        near_end = jnp.minimum((g_row + NEAR) * T, NB)
        rows = lax.broadcasted_iota(jnp.int32, (L, 1), 0) // K

        @pl.loop(g_row * T, j_here + 1)
        def _(i):
            v_all[i] = jnp.zeros((K, B), BF16)

        for col in range(N_COL):
            arrived(z_all.at[col], zb_r.at[col])

        @pl.loop(j_here + 1, near_end)
        def _(i):
            arrived(v_all.at[i], v_r.at[i])

        def z():
            return jnp.concatenate([z_all[2 * h] + z_all[2 * h + 1] for h in range(N_COL // 2)], axis=1)

        def v_of(g, count):
            return v_all[pl.ds(g * T, count * T)].reshape(count * L, B)

        g_out[:, here] = nt(z(), v_of(g_row, NEAR))
        remote(*g_copy()).start()

        for col in range(N_COL):
            arrived(inv_all.at[pl.ds(col * R, R)], inv_r.at[col])

        def form(lb):
            @pl.loop(0, jnp.minimum(T, j_here - lb * T))
            def _(l):
                arrived(u_all.at[lb * T + l], u_r.at[lb * T + l])

            wl = nt(u_all[pl.ds(lb * T, T)].reshape(L, B), inv_all[...])
            wl = jnp.where(rows + lb * T < j_here, wl, 0.0).astype(BF16)
            w[lb] = wl
            m_out[lb, :, here] = nt(wl, v_of(g_row, NEAR)).astype(BF16)

        form(g_row)

        @pl.loop(0, t_row)
        def _(s):
            remote(*own_copy(s)).start()

        @pl.loop(0, g_row)
        def _(lb):
            form(lb)
            remote(*m_copy(lb)).start()

        @pl.loop(near_end, NB)
        def _(i):
            arrived(v_all.at[i], v_r.at[i])

        @pl.loop(0, (NG - NEAR + 1 - g_row) // 2)
        def _(h):
            far = g_row + NEAR + 2 * h
            cols = lanes_of(far, 2)
            g_out[:, cols] = nt(z(), v_of(far, 2))

            @pl.loop(0, g_row + 1)
            def _(lb):
                m_out[lb, :, cols] = nt(w[lb], v_of(far, 2)).astype(BF16)

    def p_chain_copy(g):
        return (p_out.at[g], p_in.at[g_here], pc_s.at[g], pc_r.at[g_here], *chain_place(g))

    def p_row_copy(g, i):
        return (p_out.at[g, i], p_row.at[g_here], pr_s.at[g, i], pr_r.at[g_here], *row_place(g * T + i))

    def relay_copy(lb, i):
        return (p_in.at[lb, i], p_row.at[lb], relay_s.at[lb, i], pr_r.at[lb], *row_place(g_here * T + i))

    @pl.when(is_chain)
    def _():
        quarter = lax.broadcasted_iota(jnp.int32, (R, L), 1) // K
        last = jnp.maximum(g_here - 1, 0)

        def across(parts):
            gives = []
            for i in range(T):
                row = parts[0] if i == 0 else pltpu.roll(parts[0], (L - K * i) % L, 1)
                for t in range(1, T):
                    shift = (K * (t - i)) % L
                    row = jnp.where(quarter == t, parts[t] if shift == 0 else pltpu.roll(parts[t], shift, 1), row)
                gives.append(row)
            return gives

        for s in range(T):
            for t in range(s + 1, T):
                for i in range(T):
                    if i != t:
                        m_own[s, t, i * K:(i + 1) * K, :] = jnp.zeros((K, WIDE), BF16)

        @pl.when(g_here == 0)
        def _():
            p_in[0] = jnp.zeros((T, R, L), BF16)
            for t in range(T):
                m_in[t, 0] = jnp.zeros((L, WIDE), BF16)

        here = lanes_of(g_here, NEAR)
        now = lanes_of(g_here, 2)

        def wait_m(lb):
            for t in range(T):
                arrived(m_in.at[t, lb, :, here], m_r.at[t, lb])

        def update(lb):
            wait_m(lb)
            for t in range(T):
                acc[t, :, here] = acc[t, :, here] - nn(p_in[lb, t], m_in[t, lb, :, here])

        for t in range(T):
            arrived(acc.at[t, :, here], g_r.at[t])
            for s in range(t):
                arrived(m_own.at[s, t, pl.ds(t * K, K), here], own_r.at[s, t])

        @pl.loop(0, g_here - NEAR + 1)
        def _(lb):
            for t in range(T):
                arrived(s_in.at[lb, t], s_r.at[lb, t])
            for i, block in enumerate(across([s_in[lb, t].astype(F32) for t in range(T)])):
                p_in[lb, i] = block.astype(BF16)
            for i in range(T):
                remote(*relay_copy(lb, i)).start()
            update(lb)

        @pl.when(g_here > 1)
        def _():
            arrived(p_in.at[g_here - 2], pc_r.at[g_here - 2])
            update(g_here - 2)

        @pl.when(g_here > 0)
        def _():
            wait_m(last)
            arrived(p_in.at[last], pc_r.at[last])

        found, inner = [], []
        for t in range(T):
            x = acc[t, :, now] - nn(p_in[last, t], m_in[t, last, :, now])
            for s in range(t):
                x = x - nn(inner[s], m_own[s, t, :, now])
            found.append(x)
            inner.append(x[:, :L].astype(BF16))

        @pl.when(g_here < NG - 1)
        def _():
            for i, block in enumerate(across([x[:, L:] for x in found])):
                p_out[g_here + 1, i] = block.astype(BF16)
            remote(*p_chain_copy(g_here + 1)).start()

        for i, block in enumerate(across([x[:, :L] for x in found])):
            p_out[g_here, i] = jnp.where(quarter < i, block, 0.0).astype(BF16)
            remote(*p_row_copy(g_here, i)).start()

        @pl.when(g_here < NG - 1)
        def _():
            for i in range(T):
                remote(*p_row_copy(g_here + 1, i)).start()

        @pl.when(g_here < NG - 2)
        def _():
            cols = lanes_of(g_here + 2, 1)
            later = []
            for t in range(T):
                x = acc[t, :, cols] - nn(p_in[last, t], m_in[t, last, :, cols])
                for s in range(t):
                    x = x - nn(inner[s], m_own[s, t, :, cols])
                later.append(x)
            for i, block in enumerate(across(later)):
                p_out[g_here + 2, i] = block.astype(BF16)
            remote(*p_chain_copy(g_here + 2)).start()
            for i in range(T):
                remote(*p_row_copy(g_here + 2, i)).start()

    @pl.when(is_row)
    def _():
        def term(g):
            arrived(p_row.at[g], pr_r.at[g])
            p = p_row[g]

            @pl.loop(0, (NG - NEAR + 1 - g_row) // 2)
            def _(h):
                cols = lanes_of(g_row + NEAR + 2 * h, 2)
                g_out[:, cols] = g_out[:, cols] - nn(p, m_out[g, :, cols])

            @pl.when(g == g_row)
            def _():
                @pl.loop(g_row + NEAR, NG)
                def _(far):
                    s_out[far] = g_out[:, lanes_of(far, 1)].astype(BF16)
                    remote(*slab_copy(far)).start()

            return nn(p, w[g])

        correction = lax.fori_loop(0, g_row + 1, lambda g, total: total + term(g), jnp.zeros((R, B), F32))
        c_out[...] = correction.astype(BF16)
        for step in (3, 4, 1, 2, 5, 6, 7, 0):
            send(*c_copy((q + step) % N_COL))

    for col in range(N_COL):
        arrived(zf.at[col], zf_r.at[col])
    for a in range(2):
        z = jnp.concatenate([zf[col][:, a * R:(a + 1) * R] for col in range(N_COL)], axis=1)
        arrived(c_in.at[a], c_r.at[a])
        out[a] = z - c_in[a].astype(F32)

    second_wave(sent)
    each_v(sent, False, range(BC))
    for step in range(1, N_COL):
        sent(*zf_copy(step))

    @pl.when(is_row)
    def _():
        remote(*g_copy()).wait_send()

        @pl.loop(0, g_row)
        def _(lb):
            remote(*m_copy(lb)).wait_send()

        @pl.loop(0, t_row)
        def _(s):
            remote(*own_copy(s)).wait_send()

        @pl.loop(g_row + NEAR, NG)
        def _(far):
            remote(*slab_copy(far)).wait_send()

        for col in range(N_COL):
            sent(*c_copy(col))

    @pl.when(is_chain)
    def _():
        upto = jnp.minimum(g_here + NEAR, NG)

        @pl.loop(g_here, upto)
        def _(g):
            for i in range(T):
                remote(*p_row_copy(g, i)).wait_send()

        @pl.loop(g_here + 1, upto)
        def _(g):
            remote(*p_chain_copy(g)).wait_send()

        @pl.loop(0, g_here - NEAR + 1)
        def _(lb):
            for i in range(T):
                remote(*relay_copy(lb, i)).wait_send()


def on_device(rhs, inverse_t, u_factors, v_factors, tile_ranks):
    vmem = pl.BlockSpec(memory_space=pltpu.VMEM)
    hbm = pl.BlockSpec(memory_space=pl.ANY)
    dma = pltpu.SemaphoreType.DMA
    solved = pl.pallas_call(
        kernel,
        out_shape=jax.ShapeDtypeStruct((2, R, B), F32),
        in_specs=[pl.BlockSpec(memory_space=pltpu.SMEM), hbm, hbm, hbm, hbm],
        out_specs=vmem,
        scratch_shapes=[
            pltpu.VMEM((2, R, B), F32),
            pltpu.VMEM((2, R, B), F32),
            pltpu.VMEM((2, BC, K, B), BF16),
            pltpu.VMEM((2, BC, K, B), BF16),
            pltpu.VMEM((2, BC, K, B), BF16),
            pltpu.VMEM((2, R, B), BF16),
            pltpu.VMEM((R, 2 * R), F32),
            pltpu.VMEM((2, R, 2 * R), BF16),
            pltpu.VMEM((N_COL, R, 2 * R), F32),
            pltpu.VMEM((B, B), BF16),
            pltpu.VMEM((NB, K, B), BF16),
            pltpu.VMEM((NB + 2 * T, K, B), BF16),
            pltpu.VMEM((N_COL, R, 2 * R), BF16),
            pltpu.VMEM((NG, L, B), BF16),
            pltpu.VMEM((NG, L, WIDE), BF16),
            pltpu.VMEM((R, WIDE), F32),
            pltpu.VMEM((NG, R, L), BF16),
            pltpu.VMEM((NG, R, L), BF16),
            pltpu.VMEM((R, B), BF16),
            pltpu.VMEM((2, R, B), BF16),
            pltpu.VMEM((T, NG, L, WIDE), BF16),
            pltpu.VMEM((T, T, L, WIDE), BF16),
            pltpu.VMEM((T, R, WIDE), F32),
            pltpu.VMEM((NG, T, R, L), BF16),
            pltpu.VMEM((NG, T, R, L), BF16),
            pltpu.VMEM((NG, T, R, L), BF16),
            dma((4,)), dma((2,)), dma((2, BC)), dma((2, BC)), dma((2,)), dma((N_COL,)),
            dma((NG,)), dma((T,)), dma((1,)), dma((NG,)), dma((NG,)), dma((NG, T)), dma((NG, T)), dma((N_COL,)),
            dma((N_COL,)), dma((NB,)), dma((NB,)), dma((N_COL,)), dma((N_COL,)),
            dma((T, NG)), dma((T, T)), dma((T,)), dma((NG, T)), dma((NG,)), dma((NG,)), dma((2,)),
        ],
        compiler_params=pltpu.CompilerParams(has_side_effects=True, collective_id=0),
    )(
        tile_ranks[:, 0, :, 0], rhs[:, 0], jnp.swapaxes(inverse_t[:, 0], 1, 2),
        u_factors[:, 0, :, 0], v_factors[:, 0, :, 0],
    )
    return solved[:, None]


def solution(mesh):
    in_specs = (
        P(None, "row", None, None),
        P(None, "row", None, "col"),
        P(None, "row", None, "col", None, None),
        P(None, "row", None, "col", None, None),
        P(None, "row", None, "col"),
    )
    out_specs = P(None, "row", None, None)
    return jax.shard_map(
        on_device, mesh=mesh, in_specs=in_specs, out_specs=out_specs, check_vma=False
    )
```

```python
import jax
import jax.numpy as jnp
from jax import lax
from jax.experimental import pallas as pl
from jax.experimental.pallas import tpu as pltpu
from jax.sharding import PartitionSpec as P

B = 512
R = 64
K = 32
BC = 4
N_ROW = 16
N_COL = 8
NB = 32
T = 4
NG = NB // T
L = T * K
NEAR = 3
WIDE = L * (NG + NEAR - 1)
F32 = jnp.float32
BF16 = jnp.bfloat16
MESH = pl.DeviceIdType.MESH


def nn(a, b):
    return jnp.dot(a, b, preferred_element_type=F32)


def nt(a, b, precision=None):
    return lax.dot_general(a, b, (((1,), (1,)), ((), ())), precision=precision, preferred_element_type=F32)


def row_place(j):
    x = ((j % 8) // 2 + 2 * (j // N_ROW)) % 4
    return j % N_ROW, 2 * x + 1


def chain_place(g):
    late = g // 4
    return ((g + 3 * late) % 4) * 4 + 1 + late, 2 * (1 + late) + 1


def kernel(
    ranks, rhs_hbm, inv_hbm, u_hbm, v_hbm, z_out, c_in,
    rhs, inv, u, v, um, invt, zp, zpb, zf,
    inv_all, u_all, v_all, z_all, w, m_out, g_out, p_row, s_out, c_out, z_full,
    m_in, m_own, acc, s_in, p_in, p_out,
    in_s, out_s, inv_s, u_s, v_s, zb_s, zf_s, m_s, own_s, g_s, s_s, pc_s, pr_s, relay_s, c_s,
    inv_r, u_r, v_r, zb_r, zf_r, m_r, own_r, g_r, s_r, pc_r, pr_r, c_r,
):
    r = lax.axis_index("row")
    q = lax.axis_index("col")

    q_odd = q % 2 == 1
    x_here = q // 2
    late_row = jnp.where((x_here - (r % 8) // 2) % 4 == 2, 1, 0)
    j_here = r + N_ROW * late_row
    is_row = q_odd & ((x_here - (r % 8) // 2) % 2 == 0)
    g_row = j_here // T
    t_row = j_here % T
    late_chain = jnp.where(r % 4 == 2, 1, 0)
    g_here = (r // 4 + late_chain) % 4 + 4 * late_chain
    is_chain = q_odd & (x_here == 1 + late_chain) & (r % 4 == 1 + late_chain)

    def is_me(row, col):
        return (row == r) & (col == q)

    def remote(src, dst, ssem, rsem, row, col):
        return pltpu.make_async_remote_copy(
            src_ref=src, dst_ref=dst, send_sem=ssem, recv_sem=rsem,
            device_id=(row, col), device_id_type=MESH,
        )

    def send(src, dst, ssem, rsem, row, col):
        me = is_me(row, col)

        @pl.when(me)
        def _():
            pltpu.make_async_copy(src, dst, rsem).start()

        @pl.when(jnp.logical_not(me))
        def _():
            remote(src, dst, ssem, rsem, row, col).start()

    def sent(src, dst, ssem, rsem, row, col):
        @pl.when(jnp.logical_not(is_me(row, col)))
        def _():
            remote(src, dst, ssem, rsem, row, col).wait_send()

    def arrived(dst, rsem):
        pltpu.make_async_copy(dst, dst, rsem).wait()

    barrier = pltpu.get_barrier_semaphore()

    def greet(row, col):
        @pl.when(jnp.logical_not(is_me(row, col)))
        def _():
            pl.semaphore_signal(barrier, inc=1, device_id=(row, col), device_id_type=MESH)

    for step in range(1, N_COL):
        greet(r, (q + step) % N_COL)

    @pl.when(is_row)
    def _():
        @pl.loop(0, N_ROW)
        def _(row):
            greet(row, j_here % N_COL)

        @pl.loop(jnp.maximum(g_row - NEAR + 1, 0), g_row + 1)
        def _(g):
            greet(*chain_place(g))

    @pl.when(is_chain)
    def _():
        for t in range(T):
            greet(*row_place(g_here * T + t))

        @pl.loop(jnp.maximum(g_here - NEAR + 1, 0), g_here)
        def _(g):
            greet(*chain_place(g))

        @pl.loop(0, T * (g_here - NEAR + 1))
        def _(j):
            greet(*row_place(j))

    expected = N_COL - 1
    for c in range(BC):
        expected += jnp.where(is_me(*row_place(8 * c + q)), 0, 1)
    expected += jnp.where(is_row, 1 + jnp.maximum(NG - NEAR - g_row, 0), 0)
    after = jnp.minimum(NEAR - 1, NG - 1 - g_here)
    expected += jnp.where(is_chain, after + T * (after + 1), 0)

    def inv_copy(a):
        return (
            invt.at[a], inv_all.at[pl.ds(pl.multiple_of(q * R, R), R)],
            inv_s.at[a], inv_r.at[q], *row_place(N_ROW * a + r),
        )

    def u_copy(a, c):
        return (um.at[a, c], u_all.at[8 * c + q], u_s.at[a, c], u_r.at[8 * c + q], *row_place(N_ROW * a + r))

    def v_copy(a, c):
        return (v.at[a, c], v_all.at[N_ROW * a + r], v_s.at[a, c], v_r.at[N_ROW * a + r], *row_place(8 * c + q))

    def below(a, c):
        return 8 * c + q < N_ROW * a + r

    def zb_copy(a):
        return (zpb.at[a], z_all.at[q], zb_s.at[a], zb_r.at[q], *row_place(N_ROW * a + r))

    def zf_copy(step):
        return (zp, zf.at[q], zf_s.at[step], zf_r.at[q], r, (q + step) % N_COL)

    loads = [
        pltpu.make_async_copy(src, dst, in_s.at[k])
        for k, (src, dst) in enumerate([(inv_hbm, inv), (rhs_hbm, rhs), (v_hbm, v), (u_hbm, u)])
    ]
    for load in loads:
        load.start()
    loads[0].wait()
    invt[...] = inv[...].astype(BF16)
    loads[1].wait()
    z_mine = [nt(rhs[a], inv[a], lax.Precision.HIGHEST) for a in range(2)]
    zp[...] = jnp.concatenate(z_mine, axis=1)
    for a in range(2):
        wide = jnp.concatenate([z_mine[a], z_mine[a]], axis=1)
        keep = lax.broadcasted_iota(jnp.int32, (R, 2 * R), 1) // R == q % 2
        zpb[a] = jnp.where(keep, wide, 0.0).astype(BF16)

    pl.semaphore_wait(barrier, expected)

    def near(a, c):
        return (N_ROW * a + r) // T - (8 * c + q) // T < NEAR

    def each_v(do, wanted, columns):
        for c in columns:
            for a in range(2):
                @pl.when(below(a, c) & (near(a, c) == wanted))
                def _(a=a, c=c):
                    do(*v_copy(a, c))

    def each_u(do, a):
        for c in range(BC):
            @pl.when(below(a, c))
            def _(c=c):
                do(*u_copy(a, c))

    def first_wave(do):
        do(*zb_copy(0))
        do(*zb_copy(1))
        do(*inv_copy(0))
        each_v(do, True, (0, 1))

    def second_wave(do):
        each_v(do, True, (2, 3))
        do(*inv_copy(1))
        each_u(do, 1)

    def mask_u(a):
        rank_rows = lax.broadcasted_iota(jnp.int32, (K, B), 0)
        for c in range(BC):
            um[a, c] = jnp.where(rank_rows < ranks[a, c], u[a, c].astype(F32), 0.0).astype(BF16)

    loads[2].wait()
    first_wave(send)
    loads[3].wait()
    mask_u(0)
    each_u(send, 0)
    mask_u(1)
    first_wave(sent)
    each_v(send, False, (0,))
    second_wave(send)
    each_v(send, False, (1, 2, 3))
    for step in range(N_COL):
        send(*zf_copy(step))

    def lanes_of(g, count):
        return pl.ds(pl.multiple_of(g * L, L), count * L)

    def by_width(g, do):
        for count in range(1, NEAR + 1):
            @pl.when(jnp.minimum(NEAR, NG - g) == count)
            def _(count=count):
                do(count)

    def m_copy(lb, count):
        lanes = lanes_of(g_row, count)
        return (
            m_out.at[lb, :, lanes], m_in.at[t_row, lb, :, lanes],
            m_s.at[lb], m_r.at[t_row, lb], *chain_place(g_row),
        )

    def own_copy(s, count):
        lanes = lanes_of(g_row, count)
        return (
            m_out.at[g_row, pl.ds(s * K, K), lanes],
            m_own.at[s, t_row, pl.ds(pl.multiple_of(t_row * K, K), K), lanes],
            own_s.at[s], own_r.at[s, t_row], *chain_place(g_row),
        )

    def g_copy(count):
        lanes = lanes_of(g_row, count)
        return (
            g_out.at[:, lanes], acc.at[t_row, :, lanes],
            g_s.at[0], g_r.at[t_row], *chain_place(g_row),
        )

    def slab_copy(g):
        return (s_out.at[g], s_in.at[g_row, t_row], s_s.at[g], s_r.at[g_row, t_row], *chain_place(g))

    def c_copy(col):
        return (c_out, c_in.at[j_here // N_ROW], c_s.at[col], c_r.at[j_here // N_ROW], r, col)

    @pl.when(is_row)
    def _():
        here = lanes_of(g_row, NEAR)
        near_end = jnp.minimum((g_row + NEAR) * T, NB)
        rows = lax.broadcasted_iota(jnp.int32, (L, 1), 0) // K

        @pl.loop(g_row * T, j_here + 1)
        def _(i):
            v_all[i] = jnp.zeros((K, B), BF16)

        for col in range(N_COL):
            arrived(z_all.at[col], zb_r.at[col])

        @pl.loop(j_here + 1, near_end)
        def _(i):
            arrived(v_all.at[i], v_r.at[i])

        def z():
            return jnp.concatenate([z_all[2 * h] + z_all[2 * h + 1] for h in range(N_COL // 2)], axis=1)

        def v_of(g, count):
            return v_all[pl.ds(g * T, count * T)].reshape(count * L, B)

        g_out[:, here] = nt(z(), v_of(g_row, NEAR))
        by_width(g_row, lambda count: remote(*g_copy(count)).start())

        for col in range(N_COL):
            arrived(inv_all.at[pl.ds(col * R, R)], inv_r.at[col])

        def form(lb):
            @pl.loop(0, jnp.minimum(T, j_here - lb * T))
            def _(l):
                arrived(u_all.at[lb * T + l], u_r.at[lb * T + l])

            wl = nt(u_all[pl.ds(lb * T, T)].reshape(L, B), inv_all[...])
            wl = jnp.where(rows + lb * T < j_here, wl, 0.0).astype(BF16)
            w[lb] = wl
            m_out[lb, :, here] = nt(wl, v_of(g_row, NEAR)).astype(BF16)

        form(g_row)

        @pl.loop(0, t_row)
        def _(s):
            by_width(g_row, lambda count: remote(*own_copy(s, count)).start())

        @pl.loop(0, g_row)
        def _(lb):
            form(lb)
            by_width(g_row, lambda count: remote(*m_copy(lb, count)).start())

        @pl.loop(near_end, NB)
        def _(i):
            arrived(v_all.at[i], v_r.at[i])

        @pl.loop(0, (NG - NEAR + 1 - g_row) // 2)
        def _(h):
            far = g_row + NEAR + 2 * h
            cols = lanes_of(far, 2)
            g_out[:, cols] = nt(z(), v_of(far, 2))

            @pl.loop(0, g_row + 1)
            def _(lb):
                m_out[lb, :, cols] = nt(w[lb], v_of(far, 2)).astype(BF16)

    def join_z():
        for col in range(N_COL):
            arrived(zf.at[col], zf_r.at[col])
        for a in range(2):
            z_full[a] = jnp.concatenate([zf[col][:, a * R:(a + 1) * R] for col in range(N_COL)], axis=1)
        pltpu.make_async_copy(z_full, z_out, out_s.at[0]).start()

    def p_chain_copy(g):
        return (p_out.at[g], p_in.at[g_here], pc_s.at[g], pc_r.at[g_here], *chain_place(g))

    def p_row_copy(g, i):
        return (p_out.at[g, i], p_row.at[g_here], pr_s.at[g, i], pr_r.at[g_here], *row_place(g * T + i))

    def relay_copy(lb, i):
        return (p_in.at[lb, i], p_row.at[lb], relay_s.at[lb, i], pr_r.at[lb], *row_place(g_here * T + i))

    @pl.when(is_chain)
    def _():
        quarter = lax.broadcasted_iota(jnp.int32, (R, L), 1) // K
        last = jnp.maximum(g_here - 1, 0)

        def across(parts):
            gives = []
            for i in range(T):
                row = parts[0] if i == 0 else pltpu.roll(parts[0], (L - K * i) % L, 1)
                for t in range(1, T):
                    shift = (K * (t - i)) % L
                    row = jnp.where(quarter == t, parts[t] if shift == 0 else pltpu.roll(parts[t], shift, 1), row)
                gives.append(row)
            return gives

        for s in range(T):
            for t in range(s + 1, T):
                for i in range(T):
                    if i != t:
                        m_own[s, t, i * K:(i + 1) * K, :] = jnp.zeros((K, WIDE), BF16)

        @pl.when(g_here == 0)
        def _():
            p_in[0] = jnp.zeros((T, R, L), BF16)
            for t in range(T):
                m_in[t, 0] = jnp.zeros((L, WIDE), BF16)

        here = lanes_of(g_here, NEAR)
        now = lanes_of(g_here, 2)

        def wait_m(lb):
            def of(count):
                for t in range(T):
                    arrived(m_in.at[t, lb, :, lanes_of(g_here, count)], m_r.at[t, lb])

            by_width(g_here, of)

        def update(lb):
            wait_m(lb)
            for t in range(T):
                acc[t, :, here] = acc[t, :, here] - nn(p_in[lb, t], m_in[t, lb, :, here])

        def wait_start(count):
            lanes = lanes_of(g_here, count)
            for t in range(T):
                arrived(acc.at[t, :, lanes], g_r.at[t])
                for s in range(t):
                    arrived(m_own.at[s, t, pl.ds(t * K, K), lanes], own_r.at[s, t])

        by_width(g_here, wait_start)

        @pl.loop(0, g_here - NEAR + 1)
        def _(lb):
            for t in range(T):
                arrived(s_in.at[lb, t], s_r.at[lb, t])
            for i, block in enumerate(across([s_in[lb, t].astype(F32) for t in range(T)])):
                p_in[lb, i] = block.astype(BF16)
            for i in range(T):
                remote(*relay_copy(lb, i)).start()
            update(lb)

        @pl.loop(jnp.maximum(g_here - NEAR + 1, 0), g_here - 1)
        def _(lb):
            arrived(p_in.at[lb], pc_r.at[lb])
            update(lb)

        @pl.when(g_here > 0)
        def _():
            wait_m(last)
            arrived(p_in.at[last], pc_r.at[last])

        found, inner = [], []
        for t in range(T):
            x = acc[t, :, now] - nn(p_in[last, t], m_in[t, last, :, now])
            for s in range(t):
                x = x - nn(inner[s], m_own[s, t, :, now])
            found.append(x)
            inner.append(x[:, :L].astype(BF16))

        @pl.when(g_here < NG - 1)
        def _():
            for i, block in enumerate(across([x[:, L:] for x in found])):
                p_out[g_here + 1, i] = block.astype(BF16)
            remote(*p_chain_copy(g_here + 1)).start()

        for i, block in enumerate(across([x[:, :L] for x in found])):
            if i > 0:
                p_out[g_here, i] = jnp.where(quarter < i, block, 0.0).astype(BF16)
                remote(*p_row_copy(g_here, i)).start()

        @pl.when(g_here < NG - 1)
        def _():
            for i in range(T):
                remote(*p_row_copy(g_here + 1, i)).start()

        for ahead in range(2, NEAR):
            @pl.when(g_here < NG - ahead)
            def _(ahead=ahead):
                cols = lanes_of(g_here + ahead, 1)
                later = []
                for t in range(T):
                    x = acc[t, :, cols] - nn(p_in[last, t], m_in[t, last, :, cols])
                    for s in range(t):
                        x = x - nn(inner[s], m_own[s, t, :, cols])
                    later.append(x)
                for i, block in enumerate(across(later)):
                    p_out[g_here + ahead, i] = block.astype(BF16)
                remote(*p_chain_copy(g_here + ahead)).start()
                for i in range(T):
                    remote(*p_row_copy(g_here + ahead, i)).start()

    @pl.when(is_row)
    def _():
        join_z()

        blocks = g_row + jnp.where(t_row > 0, 1, 0)

        def send_slabs():
            @pl.loop(g_row + NEAR, NG)
            def _(far):
                s_out[far] = g_out[:, lanes_of(far, 1)].astype(BF16)
                remote(*slab_copy(far)).start()

        def term(g):
            arrived(p_row.at[g], pr_r.at[g])
            p = p_row[g]

            @pl.loop(0, (NG - NEAR + 1 - g_row) // 2)
            def _(h):
                cols = lanes_of(g_row + NEAR + 2 * h, 2)
                g_out[:, cols] = g_out[:, cols] - nn(p, m_out[g, :, cols])

            @pl.when(g == blocks - 1)
            def _():
                send_slabs()

            return nn(p, w[g])

        @pl.when(blocks == 0)
        def _():
            send_slabs()

        correction = lax.fori_loop(0, blocks, lambda g, total: total + term(g), jnp.zeros((R, B), F32))
        c_out[...] = correction.astype(BF16)
        for step in (3, 4, 1, 2, 5, 6, 7, 0):
            send(*c_copy((q + step) % N_COL))

    @pl.when(jnp.logical_not(is_row))
    def _():
        join_z()

    pltpu.make_async_copy(z_full, z_out, out_s.at[0]).wait()
    for a in range(2):
        arrived(c_in.at[a], c_r.at[a])

    each_u(sent, 0)
    second_wave(sent)
    each_v(sent, False, range(BC))
    for step in range(1, N_COL):
        sent(*zf_copy(step))

    @pl.when(is_row)
    def _():
        by_width(g_row, lambda count: remote(*g_copy(count)).wait_send())

        @pl.loop(0, g_row)
        def _(lb):
            by_width(g_row, lambda count: remote(*m_copy(lb, count)).wait_send())

        @pl.loop(0, t_row)
        def _(s):
            by_width(g_row, lambda count: remote(*own_copy(s, count)).wait_send())

        @pl.loop(g_row + NEAR, NG)
        def _(far):
            remote(*slab_copy(far)).wait_send()

        for col in range(N_COL):
            sent(*c_copy(col))

    @pl.when(is_chain)
    def _():
        upto = jnp.minimum(g_here + NEAR, NG)

        for i in range(1, T):
            remote(*p_row_copy(g_here, i)).wait_send()

        @pl.loop(g_here + 1, upto)
        def _(g):
            for i in range(T):
                remote(*p_row_copy(g, i)).wait_send()

        @pl.loop(g_here + 1, upto)
        def _(g):
            remote(*p_chain_copy(g)).wait_send()

        @pl.loop(0, g_here - NEAR + 1)
        def _(lb):
            for i in range(T):
                remote(*relay_copy(lb, i)).wait_send()


def on_device(rhs, inverse_t, u_factors, v_factors, tile_ranks):
    hbm = pl.BlockSpec(memory_space=pl.ANY)
    dma = pltpu.SemaphoreType.DMA
    z, c = pl.pallas_call(
        kernel,
        out_shape=(jax.ShapeDtypeStruct((2, R, B), F32), jax.ShapeDtypeStruct((2, R, B), BF16)),
        in_specs=[pl.BlockSpec(memory_space=pltpu.SMEM), hbm, hbm, hbm, hbm],
        out_specs=(hbm, hbm),
        scratch_shapes=[
            pltpu.VMEM((2, R, B), F32),
            pltpu.VMEM((2, R, B), F32),
            pltpu.VMEM((2, BC, K, B), BF16),
            pltpu.VMEM((2, BC, K, B), BF16),
            pltpu.VMEM((2, BC, K, B), BF16),
            pltpu.VMEM((2, R, B), BF16),
            pltpu.VMEM((R, 2 * R), F32),
            pltpu.VMEM((2, R, 2 * R), BF16),
            pltpu.VMEM((N_COL, R, 2 * R), F32),
            pltpu.VMEM((B, B), BF16),
            pltpu.VMEM((NB, K, B), BF16),
            pltpu.VMEM((NB + (NEAR - 1) * T, K, B), BF16),
            pltpu.VMEM((N_COL, R, 2 * R), BF16),
            pltpu.VMEM((NG, L, B), BF16),
            pltpu.VMEM((NG, L, WIDE), BF16),
            pltpu.VMEM((R, WIDE), F32),
            pltpu.VMEM((NG, R, L), BF16),
            pltpu.VMEM((NG, R, L), BF16),
            pltpu.VMEM((R, B), BF16),
            pltpu.VMEM((2, R, B), F32),
            pltpu.VMEM((T, NG, L, WIDE), BF16),
            pltpu.VMEM((T, T, L, WIDE), BF16),
            pltpu.VMEM((T, R, WIDE), F32),
            pltpu.VMEM((NG, T, R, L), BF16),
            pltpu.VMEM((NG, T, R, L), BF16),
            pltpu.VMEM((NG, T, R, L), BF16),
            dma((4,)), dma((1,)), dma((2,)), dma((2, BC)), dma((2, BC)), dma((2,)), dma((N_COL,)),
            dma((NG,)), dma((T,)), dma((1,)), dma((NG,)), dma((NG,)), dma((NG, T)), dma((NG, T)), dma((N_COL,)),
            dma((N_COL,)), dma((NB,)), dma((NB,)), dma((N_COL,)), dma((N_COL,)),
            dma((T, NG)), dma((T, T)), dma((T,)), dma((NG, T)), dma((NG,)), dma((NG,)), dma((2,)),
        ],
        compiler_params=pltpu.CompilerParams(has_side_effects=True, collective_id=0),
    )(
        tile_ranks[:, 0, :, 0], rhs[:, 0], jnp.swapaxes(inverse_t[:, 0], 1, 2),
        u_factors[:, 0, :, 0], v_factors[:, 0, :, 0],
    )
    return (z - c.astype(F32))[:, None]


def solution(mesh):
    in_specs = (
        P(None, "row", None, None),
        P(None, "row", None, "col"),
        P(None, "row", None, "col", None, None),
        P(None, "row", None, "col", None, None),
        P(None, "row", None, "col"),
    )
    out_specs = P(None, "row", None, None)
    return jax.shard_map(
        on_device, mesh=mesh, in_specs=in_specs, out_specs=out_specs, check_vma=False
    )
```

```python
import jax
import jax.numpy as jnp
from jax import lax
from jax.experimental import pallas as pl
from jax.experimental.pallas import tpu as pltpu
from jax.sharding import PartitionSpec as P

B = 512
R = 64
K = 32
BC = 4
N_ROW = 16
N_COL = 8
NB = 32
T = 4
NG = NB // T
L = T * K
NEAR = 3
WIDE = L * (NG + NEAR - 1)
F32 = jnp.float32
BF16 = jnp.bfloat16
MESH = pl.DeviceIdType.MESH


def nn(a, b):
    return jnp.dot(a, b, preferred_element_type=F32)


def nt(a, b, precision=None):
    return lax.dot_general(a, b, (((1,), (1,)), ((), ())), precision=precision, preferred_element_type=F32)


def row_place(j):
    x = ((j % 8) // 2 + 2 * (j // N_ROW)) % 4
    return j % N_ROW, 2 * x + 1


def chain_place(g):
    late = g // 4
    row = ((g + 0 * late) % 4) * 4 + 1 + 1 * late
    return row, 2 * (1 + 1 * late) + 1


def kernel(
    ranks, rhs_hbm, inv_hbm, u_hbm, v_hbm, z_out, c_in,
    rhs, inv, u, v, um, invt, zp, zpb, zf,
    inv_all, u_all, v_all, z_all, w, m_out, g_out, p_row, s_out, c_out, z_full,
    m_in, m_own, acc, s_in, p_in, p_out,
    in_s, out_s, inv_s, u_s, v_s, zb_s, zf_s, m_s, own_s, g_s, s_s, pc_s, pr_s, relay_s, c_s,
    inv_r, u_r, v_r, zb_r, zf_r, m_r, own_r, g_r, s_r, pc_r, pr_r, c_r,
):
    r = lax.axis_index("row")
    q = lax.axis_index("col")

    q_odd = q % 2 == 1
    x_here = q // 2
    late_row = jnp.where((x_here - (r % 8) // 2) % 4 == 2, 1, 0)
    j_here = r + N_ROW * late_row
    is_row = q_odd & ((x_here - (r % 8) // 2) % 2 == 0)
    g_row = j_here // T
    t_row = j_here % T
    z_here = r % 4
    late_chain = jnp.where((z_here == 2) & (x_here == 2), 1, 0)
    g_here = (r // 4 + 0 * late_chain) % 4 + 4 * late_chain
    is_chain = q_odd & (((z_here == 1) & (x_here == 1)) | (late_chain == 1))

    def is_me(row, col):
        return (row == r) & (col == q)

    def remote(src, dst, ssem, rsem, row, col):
        return pltpu.make_async_remote_copy(
            src_ref=src, dst_ref=dst, send_sem=ssem, recv_sem=rsem,
            device_id=(row, col), device_id_type=MESH,
        )

    def send(src, dst, ssem, rsem, row, col):
        me = is_me(row, col)

        @pl.when(me)
        def _():
            pltpu.make_async_copy(src, dst, rsem).start()

        @pl.when(jnp.logical_not(me))
        def _():
            remote(src, dst, ssem, rsem, row, col).start()

    def sent(src, dst, ssem, rsem, row, col):
        @pl.when(jnp.logical_not(is_me(row, col)))
        def _():
            remote(src, dst, ssem, rsem, row, col).wait_send()

    def arrived(dst, rsem):
        pltpu.make_async_copy(dst, dst, rsem).wait()

    barrier = pltpu.get_barrier_semaphore()

    def greet(row, col):
        @pl.when(jnp.logical_not(is_me(row, col)))
        def _():
            pl.semaphore_signal(barrier, inc=1, device_id=(row, col), device_id_type=MESH)

    for step in range(1, N_COL):
        greet(r, (q + step) % N_COL)

    @pl.when(is_row)
    def _():
        @pl.loop(0, N_ROW)
        def _(row):
            greet(row, j_here % N_COL)

        @pl.loop(jnp.maximum(g_row - NEAR + 1, 0), g_row + 1)
        def _(g):
            greet(*chain_place(g))

    @pl.when(is_chain)
    def _():
        for t in range(T):
            greet(*row_place(g_here * T + t))

        @pl.loop(jnp.maximum(g_here - NEAR + 1, 0), g_here)
        def _(g):
            greet(*chain_place(g))

        @pl.loop(0, T * (g_here - NEAR + 1))
        def _(j):
            greet(*row_place(j))

    expected = N_COL - 1
    for c in range(BC):
        expected += jnp.where(is_me(*row_place(8 * c + q)), 0, 1)
    expected += jnp.where(is_row, 1 + jnp.maximum(NG - NEAR - g_row, 0), 0)
    after = jnp.minimum(NEAR - 1, NG - 1 - g_here)
    expected += jnp.where(is_chain, after + T * (after + 1), 0)

    def inv_copy(a):
        return (
            invt.at[a], inv_all.at[pl.ds(pl.multiple_of(q * R, R), R)],
            inv_s.at[a], inv_r.at[q], *row_place(N_ROW * a + r),
        )

    def u_copy(a, c):
        return (um.at[a, c], u_all.at[8 * c + q], u_s.at[a, c], u_r.at[8 * c + q], *row_place(N_ROW * a + r))

    def v_copy(a, c):
        return (v.at[a, c], v_all.at[N_ROW * a + r], v_s.at[a, c], v_r.at[N_ROW * a + r], *row_place(8 * c + q))

    def below(a, c):
        return 8 * c + q < N_ROW * a + r

    def zb_copy(a):
        return (zpb.at[a], z_all.at[q], zb_s.at[a], zb_r.at[q], *row_place(N_ROW * a + r))

    def zf_copy(step):
        return (zp, zf.at[q], zf_s.at[step], zf_r.at[q], r, (q + step) % N_COL)

    loads = [
        pltpu.make_async_copy(src, dst, in_s.at[k])
        for k, (src, dst) in enumerate([(inv_hbm, inv), (rhs_hbm, rhs), (v_hbm, v), (u_hbm, u)])
    ]
    for load in loads:
        load.start()
    loads[0].wait()
    invt[...] = inv[...].astype(BF16)
    loads[1].wait()
    z_mine = [nt(rhs[a], inv[a], lax.Precision.HIGHEST) for a in range(2)]
    zp[...] = jnp.concatenate(z_mine, axis=1)
    for a in range(2):
        wide = jnp.concatenate([z_mine[a], z_mine[a]], axis=1)
        keep = lax.broadcasted_iota(jnp.int32, (R, 2 * R), 1) // R == q % 2
        zpb[a] = jnp.where(keep, wide, 0.0).astype(BF16)

    pl.semaphore_wait(barrier, expected)

    def near(a, c):
        return (N_ROW * a + r) // T - (8 * c + q) // T < NEAR

    def each_v(do, wanted, columns):
        for c in columns:
            for a in range(2):
                @pl.when(below(a, c) & (near(a, c) == wanted))
                def _(a=a, c=c):
                    do(*v_copy(a, c))

    def each_u(do, a):
        for c in range(BC):
            @pl.when(below(a, c))
            def _(c=c):
                do(*u_copy(a, c))

    def first_wave(do):
        do(*zb_copy(0))
        do(*zb_copy(1))
        do(*inv_copy(0))
        each_v(do, True, (0, 1))

    def second_wave(do):
        each_v(do, True, (2, 3))
        do(*inv_copy(1))
        each_u(do, 1)

    def mask_u(a):
        rank_rows = lax.broadcasted_iota(jnp.int32, (K, B), 0)
        for c in range(BC):
            um[a, c] = jnp.where(rank_rows < ranks[a, c], u[a, c].astype(F32), 0.0).astype(BF16)

    loads[2].wait()
    first_wave(send)
    loads[3].wait()
    mask_u(0)
    each_u(send, 0)
    mask_u(1)
    first_wave(sent)
    each_v(send, False, (0,))
    second_wave(send)
    each_v(send, False, (1, 2, 3))
    for step in range(N_COL):
        send(*zf_copy(step))

    def lanes_of(g, count):
        return pl.ds(pl.multiple_of(g * L, L), count * L)

    def by_width(g, do):
        for count in range(1, NEAR + 1):
            @pl.when(jnp.minimum(NEAR, NG - g) == count)
            def _(count=count):
                do(count)

    def m_copy(lb, count):
        lanes = lanes_of(g_row, count)
        return (
            m_out.at[lb, :, lanes], m_in.at[t_row, lb, :, lanes],
            m_s.at[lb], m_r.at[t_row, lb], *chain_place(g_row),
        )

    def own_copy(s, count):
        lanes = lanes_of(g_row, count)
        return (
            m_out.at[g_row, pl.ds(s * K, K), lanes],
            m_own.at[s, t_row, pl.ds(pl.multiple_of(t_row * K, K), K), lanes],
            own_s.at[s], own_r.at[s, t_row], *chain_place(g_row),
        )

    def g_copy(count):
        lanes = lanes_of(g_row, count)
        return (
            g_out.at[:, lanes], acc.at[t_row, :, lanes],
            g_s.at[0], g_r.at[t_row], *chain_place(g_row),
        )

    def slab_copy(g):
        return (s_out.at[g], s_in.at[g_row, t_row], s_s.at[g], s_r.at[g_row, t_row], *chain_place(g))

    def c_copy(col):
        return (c_out, c_in.at[j_here // N_ROW], c_s.at[col], c_r.at[j_here // N_ROW], r, col)

    @pl.when(is_row)
    def _():
        here = lanes_of(g_row, NEAR)
        near_end = jnp.minimum((g_row + NEAR) * T, NB)
        rows = lax.broadcasted_iota(jnp.int32, (L, 1), 0) // K

        @pl.loop(g_row * T, j_here + 1)
        def _(i):
            v_all[i] = jnp.zeros((K, B), BF16)

        for col in range(N_COL):
            arrived(z_all.at[col], zb_r.at[col])

        @pl.loop(j_here + 1, near_end)
        def _(i):
            arrived(v_all.at[i], v_r.at[i])

        def z():
            return jnp.concatenate([z_all[2 * h] + z_all[2 * h + 1] for h in range(N_COL // 2)], axis=1)

        def v_of(g, count):
            return v_all[pl.ds(g * T, count * T)].reshape(count * L, B)

        g_out[:, here] = nt(z(), v_of(g_row, NEAR))
        by_width(g_row, lambda count: remote(*g_copy(count)).start())

        for col in range(N_COL):
            arrived(inv_all.at[pl.ds(col * R, R)], inv_r.at[col])

        def form(lb):
            @pl.loop(0, jnp.minimum(T, j_here - lb * T))
            def _(l):
                arrived(u_all.at[lb * T + l], u_r.at[lb * T + l])

            wl = nt(u_all[pl.ds(lb * T, T)].reshape(L, B), inv_all[...])
            wl = jnp.where(rows + lb * T < j_here, wl, 0.0).astype(BF16)
            w[lb] = wl
            m_out[lb, :, here] = nt(wl, v_of(g_row, NEAR)).astype(BF16)

        form(g_row)

        @pl.loop(0, t_row)
        def _(s):
            by_width(g_row, lambda count: remote(*own_copy(s, count)).start())

        @pl.loop(0, g_row)
        def _(lb):
            form(lb)
            by_width(g_row, lambda count: remote(*m_copy(lb, count)).start())

        @pl.loop(near_end, NB)
        def _(i):
            arrived(v_all.at[i], v_r.at[i])

        @pl.loop(0, (NG - NEAR + 1 - g_row) // 2)
        def _(h):
            far = g_row + NEAR + 2 * h
            cols = lanes_of(far, 2)
            g_out[:, cols] = nt(z(), v_of(far, 2))

            @pl.loop(0, g_row + 1)
            def _(lb):
                m_out[lb, :, cols] = nt(w[lb], v_of(far, 2)).astype(BF16)

    def join_z():
        for col in range(N_COL):
            arrived(zf.at[col], zf_r.at[col])
        for a in range(2):
            z_full[a] = jnp.concatenate([zf[col][:, a * R:(a + 1) * R] for col in range(N_COL)], axis=1)
        pltpu.make_async_copy(z_full, z_out, out_s.at[0]).start()

    def p_chain_copy(g, i):
        return (p_out.at[g, i], p_in.at[g_here, i], pc_s.at[g, i], pc_r.at[g_here, i], *chain_place(g))

    def p_row_copy(g, i):
        return (p_out.at[g, i], p_row.at[g_here], pr_s.at[g, i], pr_r.at[g_here], *row_place(g * T + i))

    def relay_copy(lb, i):
        return (p_in.at[lb, i], p_row.at[lb], relay_s.at[lb, i], pr_r.at[lb], *row_place(g_here * T + i))

    @pl.when(is_chain)
    def _():
        quarter = lax.broadcasted_iota(jnp.int32, (R, L), 1) // K
        last = jnp.maximum(g_here - 1, 0)

        def across(parts):
            gives = []
            for i in range(T):
                row = parts[0] if i == 0 else pltpu.roll(parts[0], (L - K * i) % L, 1)
                for t in range(1, T):
                    shift = (K * (t - i)) % L
                    row = jnp.where(quarter == t, parts[t] if shift == 0 else pltpu.roll(parts[t], shift, 1), row)
                gives.append(row)
            return gives

        for s in range(T):
            for t in range(s + 1, T):
                for i in range(T):
                    if i != t:
                        m_own[s, t, i * K:(i + 1) * K, :] = jnp.zeros((K, WIDE), BF16)

        @pl.when(g_here == 0)
        def _():
            p_in[0] = jnp.zeros((T, R, L), BF16)
            for t in range(T):
                m_in[t, 0] = jnp.zeros((L, WIDE), BF16)

        here = lanes_of(g_here, NEAR)
        now = lanes_of(g_here, 2)

        def wait_m(lb):
            def of(count):
                for t in range(T):
                    arrived(m_in.at[t, lb, :, lanes_of(g_here, count)], m_r.at[t, lb])

            by_width(g_here, of)

        def update(lb):
            wait_m(lb)
            for t in range(T):
                acc[t, :, here] = acc[t, :, here] - nn(p_in[lb, t], m_in[t, lb, :, here])

        def wait_start(count):
            lanes = lanes_of(g_here, count)
            for t in range(T):
                arrived(acc.at[t, :, lanes], g_r.at[t])
                for s in range(t):
                    arrived(m_own.at[s, t, pl.ds(t * K, K), lanes], own_r.at[s, t])

        by_width(g_here, wait_start)

        @pl.loop(0, g_here - NEAR + 1)
        def _(lb):
            for t in range(T):
                arrived(s_in.at[lb, t], s_r.at[lb, t])
            for i, block in enumerate(across([s_in[lb, t].astype(F32) for t in range(T)])):
                p_in[lb, i] = block.astype(BF16)
            for i in range(T):
                remote(*relay_copy(lb, i)).start()
            update(lb)

        @pl.loop(jnp.maximum(g_here - NEAR + 1, 0), g_here - 1)
        def _(lb):
            for i in range(T):
                arrived(p_in.at[lb, i], pc_r.at[lb, i])
            update(lb)

        @pl.when(g_here > 0)
        def _():
            wait_m(last)

        found, inner = [], []
        for t in range(T):
            @pl.when(g_here > 0)
            def _(t=t):
                arrived(p_in.at[last, t], pc_r.at[last, t])

            x = acc[t, :, now] - nn(p_in[last, t], m_in[t, last, :, now])
            for s in range(t):
                x = x - nn(inner[s], m_own[s, t, :, now])
            found.append(x)
            inner.append(x[:, :L].astype(BF16))

        @pl.when(g_here < NG - 1)
        def _():
            for i, block in enumerate(across([x[:, L:] for x in found])):
                p_out[g_here + 1, i] = block.astype(BF16)
                remote(*p_chain_copy(g_here + 1, i)).start()

        for i, block in enumerate(across([x[:, :L] for x in found])):
            if i > 0:
                p_out[g_here, i] = jnp.where(quarter < i, block, 0.0).astype(BF16)
                remote(*p_row_copy(g_here, i)).start()

        @pl.when(g_here < NG - 1)
        def _():
            for i in range(T):
                remote(*p_row_copy(g_here + 1, i)).start()

        for ahead in range(2, NEAR):
            @pl.when(g_here < NG - ahead)
            def _(ahead=ahead):
                cols = lanes_of(g_here + ahead, 1)
                later = []
                for t in range(T):
                    x = acc[t, :, cols] - nn(p_in[last, t], m_in[t, last, :, cols])
                    for s in range(t):
                        x = x - nn(inner[s], m_own[s, t, :, cols])
                    later.append(x)
                for i, block in enumerate(across(later)):
                    p_out[g_here + ahead, i] = block.astype(BF16)
                    remote(*p_chain_copy(g_here + ahead, i)).start()
                for i in range(T):
                    remote(*p_row_copy(g_here + ahead, i)).start()

    @pl.when(is_row)
    def _():
        join_z()

        blocks = g_row + jnp.where(t_row > 0, 1, 0)

        def send_slabs(h):
            for far in (g_row + NEAR + 2 * h, g_row + NEAR + 2 * h + 1):
                @pl.when(far < NG)
                def _(far=far):
                    s_out[far] = g_out[:, lanes_of(far, 1)].astype(BF16)
                    remote(*slab_copy(far)).start()

        def term(g):
            arrived(p_row.at[g], pr_r.at[g])
            p = p_row[g]

            @pl.loop(0, (NG - NEAR + 1 - g_row) // 2)
            def _(h):
                cols = lanes_of(g_row + NEAR + 2 * h, 2)
                g_out[:, cols] = g_out[:, cols] - nn(p, m_out[g, :, cols])

                @pl.when(g == blocks - 1)
                def _():
                    send_slabs(h)

            return nn(p, w[g])

        @pl.when(blocks == 0)
        def _():
            pl.loop(0, (NG - NEAR + 1 - g_row) // 2)(send_slabs)

        correction = lax.fori_loop(0, blocks, lambda g, total: total + term(g), jnp.zeros((R, B), F32))
        c_out[...] = correction.astype(BF16)
        for step in (3, 4, 1, 2, 5, 6, 7, 0):
            send(*c_copy((q + step) % N_COL))

    @pl.when(jnp.logical_not(is_row))
    def _():
        join_z()

    pltpu.make_async_copy(z_full, z_out, out_s.at[0]).wait()
    for a in range(2):
        arrived(c_in.at[a], c_r.at[a])

    each_u(sent, 0)
    second_wave(sent)
    each_v(sent, False, range(BC))
    for step in range(1, N_COL):
        sent(*zf_copy(step))

    @pl.when(is_row)
    def _():
        by_width(g_row, lambda count: remote(*g_copy(count)).wait_send())

        @pl.loop(0, g_row)
        def _(lb):
            by_width(g_row, lambda count: remote(*m_copy(lb, count)).wait_send())

        @pl.loop(0, t_row)
        def _(s):
            by_width(g_row, lambda count: remote(*own_copy(s, count)).wait_send())

        @pl.loop(g_row + NEAR, NG)
        def _(far):
            remote(*slab_copy(far)).wait_send()

        for col in range(N_COL):
            sent(*c_copy(col))

    @pl.when(is_chain)
    def _():
        upto = jnp.minimum(g_here + NEAR, NG)

        for i in range(1, T):
            remote(*p_row_copy(g_here, i)).wait_send()

        @pl.loop(g_here + 1, upto)
        def _(g):
            for i in range(T):
                remote(*p_row_copy(g, i)).wait_send()

        @pl.loop(g_here + 1, upto)
        def _(g):
            for i in range(T):
                remote(*p_chain_copy(g, i)).wait_send()

        @pl.loop(0, g_here - NEAR + 1)
        def _(lb):
            for i in range(T):
                remote(*relay_copy(lb, i)).wait_send()


def on_device(rhs, inverse_t, u_factors, v_factors, tile_ranks):
    hbm = pl.BlockSpec(memory_space=pl.ANY)
    dma = pltpu.SemaphoreType.DMA
    z, c = pl.pallas_call(
        kernel,
        out_shape=(jax.ShapeDtypeStruct((2, R, B), F32), jax.ShapeDtypeStruct((2, R, B), BF16)),
        in_specs=[pl.BlockSpec(memory_space=pltpu.SMEM), hbm, hbm, hbm, hbm],
        out_specs=(hbm, hbm),
        scratch_shapes=[
            pltpu.VMEM((2, R, B), F32),
            pltpu.VMEM((2, R, B), F32),
            pltpu.VMEM((2, BC, K, B), BF16),
            pltpu.VMEM((2, BC, K, B), BF16),
            pltpu.VMEM((2, BC, K, B), BF16),
            pltpu.VMEM((2, R, B), BF16),
            pltpu.VMEM((R, 2 * R), F32),
            pltpu.VMEM((2, R, 2 * R), BF16),
            pltpu.VMEM((N_COL, R, 2 * R), F32),
            pltpu.VMEM((B, B), BF16),
            pltpu.VMEM((NB, K, B), BF16),
            pltpu.VMEM((NB + (NEAR - 1) * T, K, B), BF16),
            pltpu.VMEM((N_COL, R, 2 * R), BF16),
            pltpu.VMEM((NG, L, B), BF16),
            pltpu.VMEM((NG, L, WIDE), BF16),
            pltpu.VMEM((R, WIDE), F32),
            pltpu.VMEM((NG, R, L), BF16),
            pltpu.VMEM((NG, R, L), BF16),
            pltpu.VMEM((R, B), BF16),
            pltpu.VMEM((2, R, B), F32),
            pltpu.VMEM((T, NG, L, WIDE), BF16),
            pltpu.VMEM((T, T, L, WIDE), BF16),
            pltpu.VMEM((T, R, WIDE), F32),
            pltpu.VMEM((NG, T, R, L), BF16),
            pltpu.VMEM((NG, T, R, L), BF16),
            pltpu.VMEM((NG, T, R, L), BF16),
            dma((4,)), dma((1,)), dma((2,)), dma((2, BC)), dma((2, BC)), dma((2,)), dma((N_COL,)),
            dma((NG,)), dma((T,)), dma((1,)), dma((NG,)), dma((NG, T)), dma((NG, T)), dma((NG, T)), dma((N_COL,)),
            dma((N_COL,)), dma((NB,)), dma((NB,)), dma((N_COL,)), dma((N_COL,)),
            dma((T, NG)), dma((T, T)), dma((T,)), dma((NG, T)), dma((NG, T)), dma((NG,)), dma((2,)),
        ],
        compiler_params=pltpu.CompilerParams(has_side_effects=True, collective_id=0),
    )(
        tile_ranks[:, 0, :, 0], rhs[:, 0], jnp.swapaxes(inverse_t[:, 0], 1, 2),
        u_factors[:, 0, :, 0], v_factors[:, 0, :, 0],
    )
    return (z - c.astype(F32))[:, None]


def solution(mesh):
    in_specs = (
        P(None, "row", None, None),
        P(None, "row", None, "col"),
        P(None, "row", None, "col", None, None),
        P(None, "row", None, "col", None, None),
        P(None, "row", None, "col"),
    )
    out_specs = P(None, "row", None, None)
    return jax.shard_map(
        on_device, mesh=mesh, in_specs=in_specs, out_specs=out_specs, check_vma=False
    )
```

```python
import jax
import jax.numpy as jnp
from jax import lax
from jax.experimental import pallas as pl
from jax.experimental.pallas import tpu as pltpu
from jax.sharding import PartitionSpec as P

B = 512
R = 64
K = 32
BC = 4
N_ROW = 16
N_COL = 8
NB = 32
T = 4
NG = NB // T
L = T * K
NEAR = 3
WIDE = L * (NG + NEAR - 1)
F32 = jnp.float32
BF16 = jnp.bfloat16
MESH = pl.DeviceIdType.MESH


def nn(a, b):
    return jnp.dot(a, b, preferred_element_type=F32)


def nt(a, b, precision=None):
    return lax.dot_general(a, b, (((1,), (1,)), ((), ())), precision=precision, preferred_element_type=F32)


def row_place(j):
    x = ((j % 8) // 2 + 2 * (j // N_ROW)) % 4
    return j % N_ROW, 2 * x + 1


def chain_place(g):
    late = g // 4
    row = ((g + 0 * late) % 4) * 4 + 1 + 1 * late
    return row, 2 * (1 + 1 * late) + 1


def kernel(
    ranks, rhs_hbm, inv_hbm, u_hbm, v_hbm, z_out, c_in,
    rhs, inv, u, v, um, invt, zp, zpb, zf,
    inv_all, u_all, v_all, z_all, w, m_out, g_out, p_row, s_out, c_out, z_full,
    m_in, m_own, acc, s_in, p_in, p_out,
    in_s, out_s, inv_s, u_s, v_s, zb_s, zf_s, m_s, own_s, g_s, s_s, pc_s, pr_s, relay_s, c_s,
    inv_r, u_r, v_r, zb_r, zf_r, m_r, own_r, g_r, s_r, pc_r, pr_r, c_r,
):
    r = lax.axis_index("row")
    q = lax.axis_index("col")

    q_odd = q % 2 == 1
    x_here = q // 2
    late_row = jnp.where((x_here - (r % 8) // 2) % 4 == 2, 1, 0)
    j_here = r + N_ROW * late_row
    is_row = q_odd & ((x_here - (r % 8) // 2) % 2 == 0)
    g_row = j_here // T
    t_row = j_here % T
    z_here = r % 4
    late_chain = jnp.where((z_here == 2) & (x_here == 2), 1, 0)
    g_here = (r // 4 + 0 * late_chain) % 4 + 4 * late_chain
    is_chain = q_odd & (((z_here == 1) & (x_here == 1)) | (late_chain == 1))

    def is_me(row, col):
        return (row == r) & (col == q)

    def remote(src, dst, ssem, rsem, row, col):
        return pltpu.make_async_remote_copy(
            src_ref=src, dst_ref=dst, send_sem=ssem, recv_sem=rsem,
            device_id=(row, col), device_id_type=MESH,
        )

    def send(src, dst, ssem, rsem, row, col):
        me = is_me(row, col)

        @pl.when(me)
        def _():
            pltpu.make_async_copy(src, dst, rsem).start()

        @pl.when(jnp.logical_not(me))
        def _():
            remote(src, dst, ssem, rsem, row, col).start()

    def sent(src, dst, ssem, rsem, row, col):
        @pl.when(jnp.logical_not(is_me(row, col)))
        def _():
            remote(src, dst, ssem, rsem, row, col).wait_send()

    def arrived(dst, rsem):
        pltpu.make_async_copy(dst, dst, rsem).wait()

    barrier = pltpu.get_barrier_semaphore()

    def greet(row, col):
        @pl.when(jnp.logical_not(is_me(row, col)))
        def _():
            pl.semaphore_signal(barrier, inc=1, device_id=(row, col), device_id_type=MESH)

    for step in range(1, N_COL):
        greet(r, (q + step) % N_COL)

    @pl.when(is_row)
    def _():
        @pl.loop(0, N_ROW)
        def _(row):
            greet(row, j_here % N_COL)

        @pl.loop(jnp.maximum(g_row - NEAR + 1, 0), g_row + 1)
        def _(g):
            greet(*chain_place(g))

    @pl.when(is_chain)
    def _():
        for t in range(T):
            greet(*row_place(g_here * T + t))

        @pl.loop(jnp.maximum(g_here - NEAR + 1, 0), g_here)
        def _(g):
            greet(*chain_place(g))

        @pl.loop(0, T * (g_here - NEAR + 1))
        def _(j):
            greet(*row_place(j))

    expected = N_COL - 1
    for c in range(BC):
        expected += jnp.where(is_me(*row_place(8 * c + q)), 0, 1)
    expected += jnp.where(is_row, 1 + jnp.maximum(NG - NEAR - g_row, 0), 0)
    after = jnp.minimum(NEAR - 1, NG - 1 - g_here)
    expected += jnp.where(is_chain, after + T * (after + 1), 0)

    def inv_copy(a):
        return (
            invt.at[a], inv_all.at[pl.ds(pl.multiple_of(q * R, R), R)],
            inv_s.at[a], inv_r.at[0], *row_place(N_ROW * a + r),
        )

    def u_copy(a, c):
        return (um.at[a, c], u_all.at[8 * c + q], u_s.at[a, c], u_r.at[(8 * c + q) // T], *row_place(N_ROW * a + r))

    def v_copy(a, c):
        return (v.at[a, c], v_all.at[N_ROW * a + r], v_s.at[a, c], v_r.at[(N_ROW * a + r) // T], *row_place(8 * c + q))

    def below(a, c):
        return 8 * c + q < N_ROW * a + r

    def zb_copy(a):
        return (zpb.at[a], z_all.at[q], zb_s.at[a], zb_r.at[0], *row_place(N_ROW * a + r))

    def zf_copy(step):
        return (zp, zf.at[q], zf_s.at[0], zf_r.at[0], r, (q + step) % N_COL)

    loads = [
        pltpu.make_async_copy(src, dst, in_s.at[k])
        for k, (src, dst) in enumerate([(inv_hbm, inv), (rhs_hbm, rhs), (v_hbm, v), (u_hbm, u)])
    ]
    for load in loads:
        load.start()
    loads[0].wait()
    invt[...] = inv[...].astype(BF16)
    loads[1].wait()
    z_mine = [nt(rhs[a], inv[a], lax.Precision.HIGHEST) for a in range(2)]
    zp[...] = jnp.concatenate(z_mine, axis=1)
    for a in range(2):
        wide = jnp.concatenate([z_mine[a], z_mine[a]], axis=1)
        keep = lax.broadcasted_iota(jnp.int32, (R, 2 * R), 1) // R == q % 2
        zpb[a] = jnp.where(keep, wide, 0.0).astype(BF16)

    pl.semaphore_wait(barrier, expected)

    def near(a, c):
        return (N_ROW * a + r) // T - (8 * c + q) // T < NEAR

    def each_v(do, wanted, columns):
        for c in columns:
            for a in range(2):
                @pl.when(below(a, c) & (near(a, c) == wanted))
                def _(a=a, c=c):
                    do(*v_copy(a, c))

    def each_u(do, a):
        for c in range(BC):
            @pl.when(below(a, c))
            def _(c=c):
                do(*u_copy(a, c))

    def first_wave(do):
        do(*zb_copy(0))
        do(*zb_copy(1))
        do(*inv_copy(0))
        each_v(do, True, (0, 1))

    def second_wave(do):
        each_v(do, True, (2, 3))
        do(*inv_copy(1))
        each_u(do, 1)

    def mask_u(a):
        rank_rows = lax.broadcasted_iota(jnp.int32, (K, B), 0)
        for c in range(BC):
            um[a, c] = jnp.where(rank_rows < ranks[a, c], u[a, c].astype(F32), 0.0).astype(BF16)

    loads[2].wait()
    first_wave(send)
    loads[3].wait()
    mask_u(0)
    each_u(send, 0)
    mask_u(1)
    first_wave(sent)
    each_v(send, False, (0,))
    second_wave(send)
    each_v(send, False, (1, 2, 3))
    for step in range(N_COL):
        send(*zf_copy(step))

    def lanes_of(g, count):
        return pl.ds(pl.multiple_of(g * L, L), count * L)

    def by_width(g, do):
        for count in range(1, NEAR + 1):
            @pl.when(jnp.minimum(NEAR, NG - g) == count)
            def _(count=count):
                do(count)

    def m_copy(lb, count):
        lanes = lanes_of(g_row, count)
        return (
            m_out.at[lb, :, lanes], m_in.at[t_row, lb, :, lanes],
            m_s.at[lb], m_r.at[lb], *chain_place(g_row),
        )

    def own_copy(s, count):
        lanes = lanes_of(g_row, count)
        return (
            m_out.at[g_row, pl.ds(s * K, K), lanes],
            m_own.at[s, t_row, pl.ds(pl.multiple_of(t_row * K, K), K), lanes],
            own_s.at[s], own_r.at[0], *chain_place(g_row),
        )

    def g_copy(count):
        lanes = lanes_of(g_row, count)
        return (
            g_out.at[:, lanes], acc.at[t_row, :, lanes],
            g_s.at[0], g_r.at[0], *chain_place(g_row),
        )

    def slab_copy(g):
        return (s_out.at[g], s_in.at[g_row, t_row], s_s.at[g], s_r.at[g_row], *chain_place(g))

    def c_copy(col):
        return (c_out, c_in.at[j_here // N_ROW], c_s.at[0], c_r.at[j_here // N_ROW], r, col)

    @pl.when(is_row)
    def _():
        here = lanes_of(g_row, NEAR)
        rows = lax.broadcasted_iota(jnp.int32, (L, 1), 0) // K

        @pl.loop(g_row * T, j_here + 1)
        def _(i):
            v_all[i] = jnp.zeros((K, B), BF16)

        arrived(z_all, zb_r.at[0])

        for t in range(T - 1):
            @pl.when(t_row == t)
            def _(t=t):
                arrived(v_all.at[pl.ds(j_here + 1, T - 1 - t)], v_r.at[g_row])

        @pl.loop(g_row + 1, jnp.minimum(g_row + NEAR, NG))
        def _(g):
            arrived(v_all.at[pl.ds(g * T, T)], v_r.at[g])

        def z():
            return jnp.concatenate([z_all[2 * h] + z_all[2 * h + 1] for h in range(N_COL // 2)], axis=1)

        def v_of(g, count):
            return v_all[pl.ds(g * T, count * T)].reshape(count * L, B)

        g_out[:, here] = nt(z(), v_of(g_row, NEAR))
        by_width(g_row, lambda count: remote(*g_copy(count)).start())

        arrived(inv_all, inv_r.at[0])

        def form(lb):
            for count in range(1, T + 1):
                @pl.when(jnp.minimum(T, j_here - lb * T) == count)
                def _(count=count):
                    arrived(u_all.at[pl.ds(lb * T, count)], u_r.at[lb])

            wl = nt(u_all[pl.ds(lb * T, T)].reshape(L, B), inv_all[...])
            wl = jnp.where(rows + lb * T < j_here, wl, 0.0).astype(BF16)
            w[lb] = wl
            m_out[lb, :, here] = nt(wl, v_of(g_row, NEAR)).astype(BF16)

        form(g_row)

        @pl.loop(0, t_row)
        def _(s):
            by_width(g_row, lambda count: remote(*own_copy(s, count)).start())

        @pl.loop(0, g_row)
        def _(lb):
            form(lb)
            by_width(g_row, lambda count: remote(*m_copy(lb, count)).start())

        @pl.loop(g_row + NEAR, NG)
        def _(g):
            arrived(v_all.at[pl.ds(g * T, T)], v_r.at[g])

        @pl.loop(0, (NG - NEAR + 1 - g_row) // 2)
        def _(h):
            far = g_row + NEAR + 2 * h
            cols = lanes_of(far, 2)
            g_out[:, cols] = nt(z(), v_of(far, 2))

            @pl.loop(0, g_row + 1)
            def _(lb):
                m_out[lb, :, cols] = nt(w[lb], v_of(far, 2)).astype(BF16)

    def join_z():
        arrived(zf, zf_r.at[0])
        for a in range(2):
            z_full[a] = jnp.concatenate([zf[col][:, a * R:(a + 1) * R] for col in range(N_COL)], axis=1)
        pltpu.make_async_copy(z_full, z_out, out_s.at[0]).start()

    def p_chain_copy(g, i):
        return (p_out.at[g, i], p_in.at[g_here, i], pc_s.at[g], pc_r.at[g - g_here - 1, i], *chain_place(g))

    def p_row_copy(g, i):
        return (p_out.at[g, i], p_row.at[g_here], pr_s.at[g], pr_r.at[g_here], *row_place(g * T + i))

    def relay_copy(lb, i):
        return (p_in.at[lb, i], p_row.at[lb], relay_s.at[lb], pr_r.at[lb], *row_place(g_here * T + i))

    @pl.when(is_chain)
    def _():
        quarter = lax.broadcasted_iota(jnp.int32, (R, L), 1) // K
        last = jnp.maximum(g_here - 1, 0)

        def across(parts):
            gives = []
            for i in range(T):
                row = parts[0] if i == 0 else pltpu.roll(parts[0], (L - K * i) % L, 1)
                for t in range(1, T):
                    shift = (K * (t - i)) % L
                    row = jnp.where(quarter == t, parts[t] if shift == 0 else pltpu.roll(parts[t], shift, 1), row)
                gives.append(row)
            return gives

        for s in range(T):
            for t in range(s + 1, T):
                for i in range(T):
                    if i != t:
                        m_own[s, t, i * K:(i + 1) * K, :] = jnp.zeros((K, WIDE), BF16)

        @pl.when(g_here == 0)
        def _():
            p_in[0] = jnp.zeros((T, R, L), BF16)
            for t in range(T):
                m_in[t, 0] = jnp.zeros((L, WIDE), BF16)

        here = lanes_of(g_here, NEAR)
        now = lanes_of(g_here, 2)

        def wait_m(lb):
            by_width(g_here, lambda count: arrived(m_in.at[:, lb, :, lanes_of(g_here, count)], m_r.at[lb]))

        def update(lb):
            wait_m(lb)
            for t in range(T):
                acc[t, :, here] = acc[t, :, here] - nn(p_in[lb, t], m_in[t, lb, :, here])

        def wait_start(count):
            lanes = lanes_of(g_here, count)
            arrived(acc.at[:, :, lanes], g_r.at[0])
            arrived(m_own.at[0, pl.ds(0, 2), pl.ds(0, 3 * K), lanes], own_r.at[0])

        by_width(g_here, wait_start)

        @pl.loop(0, g_here - NEAR + 1)
        def _(lb):
            arrived(s_in.at[lb], s_r.at[lb])
            for i, block in enumerate(across([s_in[lb, t].astype(F32) for t in range(T)])):
                p_in[lb, i] = block.astype(BF16)
            for i in range(T):
                remote(*relay_copy(lb, i)).start()
            update(lb)

        @pl.loop(jnp.maximum(g_here - NEAR + 1, 0), g_here - 1)
        def _(lb):
            for i in range(T):
                arrived(p_in.at[lb, i], pc_r.at[g_here - lb - 1, i])
            update(lb)

        @pl.when(g_here > 0)
        def _():
            wait_m(last)

        found, inner = [], []
        for t in range(T):
            @pl.when(g_here > 0)
            def _(t=t):
                arrived(p_in.at[last, t], pc_r.at[0, t])

            x = acc[t, :, now] - nn(p_in[last, t], m_in[t, last, :, now])
            for s in range(t):
                x = x - nn(inner[s], m_own[s, t, :, now])
            found.append(x)
            inner.append(x[:, :L].astype(BF16))

        @pl.when(g_here < NG - 1)
        def _():
            for i, block in enumerate(across([x[:, L:] for x in found])):
                p_out[g_here + 1, i] = block.astype(BF16)
                remote(*p_chain_copy(g_here + 1, i)).start()

        for i, block in enumerate(across([x[:, :L] for x in found])):
            if i > 0:
                p_out[g_here, i] = jnp.where(quarter < i, block, 0.0).astype(BF16)
                remote(*p_row_copy(g_here, i)).start()

        @pl.when(g_here < NG - 1)
        def _():
            for i in range(T):
                remote(*p_row_copy(g_here + 1, i)).start()

        for ahead in range(2, NEAR):
            @pl.when(g_here < NG - ahead)
            def _(ahead=ahead):
                cols = lanes_of(g_here + ahead, 1)
                later = []
                for t in range(T):
                    x = acc[t, :, cols] - nn(p_in[last, t], m_in[t, last, :, cols])
                    for s in range(t):
                        x = x - nn(inner[s], m_own[s, t, :, cols])
                    later.append(x)
                for i, block in enumerate(across(later)):
                    p_out[g_here + ahead, i] = block.astype(BF16)
                    remote(*p_chain_copy(g_here + ahead, i)).start()
                for i in range(T):
                    remote(*p_row_copy(g_here + ahead, i)).start()

    @pl.when(is_row)
    def _():
        join_z()

        blocks = g_row + jnp.where(t_row > 0, 1, 0)

        def send_slabs(h):
            for far in (g_row + NEAR + 2 * h, g_row + NEAR + 2 * h + 1):
                @pl.when(far < NG)
                def _(far=far):
                    s_out[far] = g_out[:, lanes_of(far, 1)].astype(BF16)
                    remote(*slab_copy(far)).start()

        def term(g):
            arrived(p_row.at[g], pr_r.at[g])
            p = p_row[g]

            @pl.loop(0, (NG - NEAR + 1 - g_row) // 2)
            def _(h):
                cols = lanes_of(g_row + NEAR + 2 * h, 2)
                g_out[:, cols] = g_out[:, cols] - nn(p, m_out[g, :, cols])

                @pl.when(g == blocks - 1)
                def _():
                    send_slabs(h)

            return nn(p, w[g])

        @pl.when(blocks == 0)
        def _():
            pl.loop(0, (NG - NEAR + 1 - g_row) // 2)(send_slabs)

        correction = lax.fori_loop(0, blocks, lambda g, total: total + term(g), jnp.zeros((R, B), F32))
        c_out[...] = correction.astype(BF16)
        for step in (3, 4, 1, 2, 5, 6, 7, 0):
            send(*c_copy((q + step) % N_COL))

    @pl.when(jnp.logical_not(is_row))
    def _():
        join_z()

    pltpu.make_async_copy(z_full, z_out, out_s.at[0]).wait()
    for a in range(2):
        arrived(c_in.at[a], c_r.at[a])

    each_u(sent, 0)
    second_wave(sent)
    each_v(sent, False, range(BC))
    arrived(zf.at[pl.ds(0, N_COL - 1)], zf_s.at[0])

    @pl.when(is_row)
    def _():
        by_width(g_row, lambda count: remote(*g_copy(count)).wait_send())

        @pl.loop(0, g_row)
        def _(lb):
            by_width(g_row, lambda count: remote(*m_copy(lb, count)).wait_send())

        @pl.loop(0, t_row)
        def _(s):
            by_width(g_row, lambda count: remote(*own_copy(s, count)).wait_send())

        @pl.loop(g_row + NEAR, NG)
        def _(far):
            remote(*slab_copy(far)).wait_send()

        arrived(p_out.at[pl.ds(0, N_COL - 1)], c_s.at[0])

    @pl.when(is_chain)
    def _():
        upto = jnp.minimum(g_here + NEAR, NG)

        arrived(p_out.at[g_here, pl.ds(1, T - 1)], pr_s.at[g_here])

        @pl.loop(g_here + 1, upto)
        def _(g):
            arrived(p_out.at[g], pr_s.at[g])
            arrived(p_out.at[g], pc_s.at[g])

        @pl.loop(0, g_here - NEAR + 1)
        def _(lb):
            arrived(p_in.at[lb], relay_s.at[lb])


def on_device(rhs, inverse_t, u_factors, v_factors, tile_ranks):
    hbm = pl.BlockSpec(memory_space=pl.ANY)
    dma = pltpu.SemaphoreType.DMA
    z, c = pl.pallas_call(
        kernel,
        out_shape=(jax.ShapeDtypeStruct((2, R, B), F32), jax.ShapeDtypeStruct((2, R, B), BF16)),
        in_specs=[pl.BlockSpec(memory_space=pltpu.SMEM), hbm, hbm, hbm, hbm],
        out_specs=(hbm, hbm),
        scratch_shapes=[
            pltpu.VMEM((2, R, B), F32),
            pltpu.VMEM((2, R, B), F32),
            pltpu.VMEM((2, BC, K, B), BF16),
            pltpu.VMEM((2, BC, K, B), BF16),
            pltpu.VMEM((2, BC, K, B), BF16),
            pltpu.VMEM((2, R, B), BF16),
            pltpu.VMEM((R, 2 * R), F32),
            pltpu.VMEM((2, R, 2 * R), BF16),
            pltpu.VMEM((N_COL, R, 2 * R), F32),
            pltpu.VMEM((B, B), BF16),
            pltpu.VMEM((NB, K, B), BF16),
            pltpu.VMEM((NB + (NEAR - 1) * T, K, B), BF16),
            pltpu.VMEM((N_COL, R, 2 * R), BF16),
            pltpu.VMEM((NG, L, B), BF16),
            pltpu.VMEM((NG, L, WIDE), BF16),
            pltpu.VMEM((R, WIDE), F32),
            pltpu.VMEM((NG, R, L), BF16),
            pltpu.VMEM((NG, R, L), BF16),
            pltpu.VMEM((R, B), BF16),
            pltpu.VMEM((2, R, B), F32),
            pltpu.VMEM((T, NG, L, WIDE), BF16),
            pltpu.VMEM((T, T, L, WIDE), BF16),
            pltpu.VMEM((T, R, WIDE), F32),
            pltpu.VMEM((NG, T, R, L), BF16),
            pltpu.VMEM((NG, T, R, L), BF16),
            pltpu.VMEM((NG, T, R, L), BF16),
            dma((4,)), dma((1,)), dma((2,)), dma((2, BC)), dma((2, BC)), dma((2,)), dma((1,)),
            dma((NG,)), dma((T,)), dma((1,)), dma((NG,)), dma((NG,)), dma((NG,)), dma((NG,)), dma((1,)),
            dma((1,)), dma((NG,)), dma((NG,)), dma((1,)), dma((1,)),
            dma((NG,)), dma((1,)), dma((1,)), dma((NG,)), dma((2, T)), dma((NG,)), dma((2,)),
        ],
        compiler_params=pltpu.CompilerParams(has_side_effects=True, collective_id=0),
    )(
        tile_ranks[:, 0, :, 0], rhs[:, 0], jnp.swapaxes(inverse_t[:, 0], 1, 2),
        u_factors[:, 0, :, 0], v_factors[:, 0, :, 0],
    )
    return (z - c.astype(F32))[:, None]


def solution(mesh):
    in_specs = (
        P(None, "row", None, None),
        P(None, "row", None, "col"),
        P(None, "row", None, "col", None, None),
        P(None, "row", None, "col", None, None),
        P(None, "row", None, "col"),
    )
    out_specs = P(None, "row", None, None)
    return jax.shard_map(
        on_device, mesh=mesh, in_specs=in_specs, out_specs=out_specs, check_vma=False
    )
```

```python
import jax
import jax.numpy as jnp
from jax import lax
from jax.experimental import pallas as pl
from jax.experimental.pallas import tpu as pltpu
from jax.sharding import PartitionSpec as P

B = 512
R = 64
K = 32
BC = 4
N_ROW = 16
N_COL = 8
NB = 32
T = 4
NG = NB // T
L = T * K
NEAR = 3
WIDE = L * (NG + NEAR - 1)
F32 = jnp.float32
BF16 = jnp.bfloat16
MESH = pl.DeviceIdType.MESH


def nn(a, b):
    return jnp.dot(a, b, preferred_element_type=F32)


def nt(a, b, precision=None):
    return lax.dot_general(a, b, (((1,), (1,)), ((), ())), precision=precision, preferred_element_type=F32)


def row_place(j):
    x = ((j % 8) // 2 + 2 * (j // N_ROW)) % 4
    return j % N_ROW, 2 * x + 1


def chain_place(g):
    late = g // 4
    row = ((g + 0 * late) % 4) * 4 + 1 + 1 * late
    return row, 2 * (1 + 1 * late) + 1


def kernel(
    ranks, rhs_hbm, inv_hbm, u_hbm, v_hbm, z_out, c_in,
    rhs, inv, u, v, um, invt, zp, zpb, zf,
    inv_all, u_all, v_all, z_all, w, m_out, g_out, p_row, s_out, c_out, z_full,
    m_in, m_own, acc, s_in, p_in, p_out,
    in_s, out_s, inv_s, u_s, v_s, zb_s, zf_s, m_s, own_s, g_s, s_s, pc_s, pr_s, relay_s, c_s,
    inv_r, u_r, v_r, zb_r, zf_r, m_r, own_r, g_r, s_r, pc_r, pr_r, c_r,
):
    r = lax.axis_index("row")
    q = lax.axis_index("col")

    q_odd = q % 2 == 1
    x_here = q // 2
    late_row = jnp.where((x_here - (r % 8) // 2) % 4 == 2, 1, 0)
    j_here = r + N_ROW * late_row
    is_row = q_odd & ((x_here - (r % 8) // 2) % 2 == 0)
    g_row = j_here // T
    t_row = j_here % T
    z_here = r % 4
    late_chain = jnp.where((z_here == 2) & (x_here == 2), 1, 0)
    g_here = (r // 4 + 0 * late_chain) % 4 + 4 * late_chain
    is_chain = q_odd & (((z_here == 1) & (x_here == 1)) | (late_chain == 1))

    def is_me(row, col):
        return (row == r) & (col == q)

    def remote(src, dst, ssem, rsem, row, col):
        return pltpu.make_async_remote_copy(
            src_ref=src, dst_ref=dst, send_sem=ssem, recv_sem=rsem,
            device_id=(row, col), device_id_type=MESH,
        )

    def send(src, dst, ssem, rsem, row, col):
        me = is_me(row, col)

        @pl.when(me)
        def _():
            pltpu.make_async_copy(src, dst, rsem).start()

        @pl.when(jnp.logical_not(me))
        def _():
            remote(src, dst, ssem, rsem, row, col).start()

    def sent(src, dst, ssem, rsem, row, col):
        @pl.when(jnp.logical_not(is_me(row, col)))
        def _():
            remote(src, dst, ssem, rsem, row, col).wait_send()

    def arrived(dst, rsem):
        pltpu.make_async_copy(dst, dst, rsem).wait()

    barrier = pltpu.get_barrier_semaphore()

    def greet(row, col):
        @pl.when(jnp.logical_not(is_me(row, col)))
        def _():
            pl.semaphore_signal(barrier, inc=1, device_id=(row, col), device_id_type=MESH)

    for step in range(1, N_COL):
        greet(r, (q + step) % N_COL)

    @pl.when(is_row)
    def _():
        @pl.loop(0, N_ROW)
        def _(row):
            greet(row, j_here % N_COL)

        @pl.loop(jnp.maximum(g_row - NEAR + 1, 0), g_row + 1)
        def _(g):
            greet(*chain_place(g))

    @pl.when(is_chain)
    def _():
        for t in range(T):
            greet(*row_place(g_here * T + t))

        @pl.loop(jnp.maximum(g_here - NEAR + 1, 0), g_here)
        def _(g):
            greet(*chain_place(g))

        @pl.loop(0, T * (g_here - NEAR + 1))
        def _(j):
            greet(*row_place(j))

    expected = N_COL - 1
    for c in range(BC):
        expected += jnp.where(is_me(*row_place(8 * c + q)), 0, 1)
    expected += jnp.where(is_row, 1 + jnp.maximum(NG - NEAR - g_row, 0), 0)
    after = jnp.minimum(NEAR - 1, NG - 1 - g_here)
    expected += jnp.where(is_chain, after + T * (after + 1), 0)

    def inv_copy(a):
        return (
            invt.at[a], inv_all.at[pl.ds(pl.multiple_of(q * R, R), R)],
            inv_s.at[a], inv_r.at[0], *row_place(N_ROW * a + r),
        )

    def u_copy(a, c):
        return (um.at[a, c], u_all.at[8 * c + q], u_s.at[a, c], u_r.at[(8 * c + q) // T], *row_place(N_ROW * a + r))

    def v_copy(a, c):
        return (v.at[a, c], v_all.at[N_ROW * a + r], v_s.at[a, c], v_r.at[(N_ROW * a + r) // T], *row_place(8 * c + q))

    def below(a, c):
        return 8 * c + q < N_ROW * a + r

    def zb_copy(a):
        return (zpb.at[a], z_all.at[q], zb_s.at[a], zb_r.at[0], *row_place(N_ROW * a + r))

    def zf_copy(step):
        return (zp, zf.at[q], zf_s.at[0], zf_r.at[0], r, (q + step) % N_COL)

    loads = [
        pltpu.make_async_copy(src, dst, in_s.at[k])
        for k, (src, dst) in enumerate([(inv_hbm, inv), (rhs_hbm, rhs), (v_hbm, v), (u_hbm, u)])
    ]
    for load in loads:
        load.start()
    loads[0].wait()
    invt[...] = inv[...].astype(BF16)
    loads[1].wait()
    z_mine = [nt(rhs[a], inv[a], lax.Precision.HIGHEST) for a in range(2)]
    zp[...] = jnp.concatenate(z_mine, axis=1)
    for a in range(2):
        wide = jnp.concatenate([z_mine[a], z_mine[a]], axis=1)
        keep = lax.broadcasted_iota(jnp.int32, (R, 2 * R), 1) // R == q % 2
        zpb[a] = jnp.where(keep, wide, 0.0).astype(BF16)

    pl.semaphore_wait(barrier, expected)

    def near(a, c):
        return (N_ROW * a + r) // T - (8 * c + q) // T < NEAR

    def each_v(do, wanted, columns):
        for c in columns:
            for a in range(2):
                @pl.when(below(a, c) & (near(a, c) == wanted))
                def _(a=a, c=c):
                    do(*v_copy(a, c))

    def each_u(do, a):
        for c in range(BC):
            @pl.when(below(a, c))
            def _(c=c):
                do(*u_copy(a, c))

    def first_wave(do):
        do(*zb_copy(0))
        do(*zb_copy(1))
        do(*inv_copy(0))
        each_v(do, True, (0, 1))

    def second_wave(do):
        each_v(do, True, (2, 3))
        do(*inv_copy(1))
        each_u(do, 1)

    def mask_u(a):
        rank_rows = lax.broadcasted_iota(jnp.int32, (K, B), 0)
        for c in range(BC):
            um[a, c] = jnp.where(rank_rows < ranks[a, c], u[a, c].astype(F32), 0.0).astype(BF16)

    loads[2].wait()
    first_wave(send)
    loads[3].wait()
    mask_u(0)
    each_u(send, 0)
    mask_u(1)
    each_v(send, False, (0,))
    second_wave(send)
    each_v(send, False, (1, 2, 3))
    for step in range(N_COL):
        send(*zf_copy(step))

    def lanes_of(g, count):
        return pl.ds(pl.multiple_of(g * L, L), count * L)

    def by_width(g, do):
        for count in range(1, NEAR + 1):
            @pl.when(jnp.minimum(NEAR, NG - g) == count)
            def _(count=count):
                do(count)

    def by_need(do):
        def of(count):
            @pl.when(t_row < T - 1)
            def _():
                do(lanes_of(g_row, count))

            if count > 1:
                @pl.when(t_row == T - 1)
                def _():
                    do(lanes_of(g_row + 1, count - 1))

        by_width(g_row, of)

    half = jnp.where(t_row == T - 1, 1, 0)

    def m_copy(lb, lanes):
        return (
            m_out.at[lb, :, lanes], m_in.at[t_row, lb, :, lanes],
            m_s.at[lb], m_r.at[half, lb], *chain_place(g_row),
        )

    def own_copy(s, lanes):
        return (
            m_out.at[g_row, pl.ds(s * K, K), lanes],
            m_own.at[s, t_row, pl.ds(pl.multiple_of(t_row * K, K), K), lanes],
            own_s.at[s], own_r.at[half], *chain_place(g_row),
        )

    def g_copy(lanes):
        return (
            g_out.at[:, lanes], acc.at[t_row, :, lanes],
            g_s.at[0], g_r.at[half], *chain_place(g_row),
        )

    def slab_copy(g):
        return (s_out.at[g], s_in.at[g_row, t_row], s_s.at[g], s_r.at[g_row], *chain_place(g))

    def c_copy(col):
        return (c_out, c_in.at[j_here // N_ROW], c_s.at[0], c_r.at[j_here // N_ROW], r, col)

    @pl.when(is_row)
    def _():
        here = lanes_of(g_row, NEAR)
        rows = lax.broadcasted_iota(jnp.int32, (L, 1), 0) // K

        @pl.loop(g_row * T, j_here + 1)
        def _(i):
            v_all[i] = jnp.zeros((K, B), BF16)

        arrived(z_all, zb_r.at[0])

        for t in range(T - 1):
            @pl.when(t_row == t)
            def _(t=t):
                arrived(v_all.at[pl.ds(j_here + 1, T - 1 - t)], v_r.at[g_row])

        @pl.loop(g_row + 1, jnp.minimum(g_row + NEAR, NG))
        def _(g):
            arrived(v_all.at[pl.ds(g * T, T)], v_r.at[g])

        def z():
            return jnp.concatenate([z_all[2 * h] + z_all[2 * h + 1] for h in range(N_COL // 2)], axis=1)

        def v_of(g, count):
            return v_all[pl.ds(g * T, count * T)].reshape(count * L, B)

        g_out[:, here] = nt(z(), v_of(g_row, NEAR))
        by_need(lambda lanes: remote(*g_copy(lanes)).start())

        arrived(inv_all, inv_r.at[0])

        def form(lb):
            for count in range(1, T + 1):
                @pl.when(jnp.minimum(T, j_here - lb * T) == count)
                def _(count=count):
                    arrived(u_all.at[pl.ds(lb * T, count)], u_r.at[lb])

            wl = nt(u_all[pl.ds(lb * T, T)].reshape(L, B), inv_all[...])
            wl = jnp.where(rows + lb * T < j_here, wl, 0.0).astype(BF16)
            w[lb] = wl
            m_out[lb, :, here] = nt(wl, v_of(g_row, NEAR)).astype(BF16)

        form(g_row)

        @pl.loop(0, t_row)
        def _(s):
            by_need(lambda lanes: remote(*own_copy(s, lanes)).start())

        @pl.loop(0, g_row)
        def _(lb):
            form(lb)
            by_need(lambda lanes: remote(*m_copy(lb, lanes)).start())

        @pl.loop(g_row + NEAR, NG)
        def _(g):
            arrived(v_all.at[pl.ds(g * T, T)], v_r.at[g])

        @pl.loop(0, (NG - NEAR + 1 - g_row) // 2)
        def _(h):
            far = g_row + NEAR + 2 * h
            cols = lanes_of(far, 2)
            g_out[:, cols] = nt(z(), v_of(far, 2))

            @pl.loop(0, g_row + 1)
            def _(lb):
                m_out[lb, :, cols] = nt(w[lb], v_of(far, 2)).astype(BF16)

    def join_z():
        arrived(zf, zf_r.at[0])
        for a in range(2):
            z_full[a] = jnp.concatenate([zf[col][:, a * R:(a + 1) * R] for col in range(N_COL)], axis=1)
        pltpu.make_async_copy(z_full, z_out, out_s.at[0]).start()

    def p_chain_copy(g, i):
        return (p_out.at[g, i], p_in.at[g_here, i], pc_s.at[g], pc_r.at[g - g_here - 1, i], *chain_place(g))

    def p_row_copy(g, i):
        return (p_out.at[g, i], p_row.at[g_here], pr_s.at[g], pr_r.at[g_here], *row_place(g * T + i))

    def relay_copy(lb, i):
        return (p_in.at[lb, i], p_row.at[lb], relay_s.at[lb], pr_r.at[lb], *row_place(g_here * T + i))

    @pl.when(is_chain)
    def _():
        quarter = lax.broadcasted_iota(jnp.int32, (R, L), 1) // K
        last = jnp.maximum(g_here - 1, 0)

        def across(parts):
            gives = []
            for i in range(T):
                row = parts[0] if i == 0 else pltpu.roll(parts[0], (L - K * i) % L, 1)
                for t in range(1, T):
                    shift = (K * (t - i)) % L
                    row = jnp.where(quarter == t, parts[t] if shift == 0 else pltpu.roll(parts[t], shift, 1), row)
                gives.append(row)
            return gives

        for s in range(T):
            for t in range(s + 1, T):
                for i in range(T):
                    if i != t:
                        m_own[s, t, i * K:(i + 1) * K, :] = jnp.zeros((K, WIDE), BF16)

        @pl.when(g_here == 0)
        def _():
            p_in[0] = jnp.zeros((T, R, L), BF16)
            for t in range(T):
                m_in[t, 0] = jnp.zeros((L, WIDE), BF16)

        here = lanes_of(g_here, NEAR)
        now = lanes_of(g_here, 2)

        def wait_m(lb):
            def of(count):
                arrived(m_in.at[pl.ds(0, T - 1), lb, :, lanes_of(g_here, count)], m_r.at[0, lb])
                if count > 1:
                    arrived(m_in.at[T - 1, lb, :, lanes_of(g_here + 1, count - 1)], m_r.at[1, lb])

            by_width(g_here, of)

        def update(lb):
            wait_m(lb)
            for t in range(T):
                acc[t, :, here] = acc[t, :, here] - nn(p_in[lb, t], m_in[t, lb, :, here])

        def wait_start(count):
            lanes = lanes_of(g_here, count)
            arrived(acc.at[pl.ds(0, T - 1), :, lanes], g_r.at[0])
            arrived(m_own.at[0, 0, pl.ds(0, 3 * K), lanes], own_r.at[0])
            if count > 1:
                lanes = lanes_of(g_here + 1, count - 1)
                arrived(acc.at[T - 1, :, lanes], g_r.at[1])
                arrived(m_own.at[0, 0, pl.ds(0, 3 * K), lanes], own_r.at[1])

        by_width(g_here, wait_start)

        @pl.loop(0, g_here - NEAR + 1)
        def _(lb):
            arrived(s_in.at[lb], s_r.at[lb])
            for i, block in enumerate(across([s_in[lb, t].astype(F32) for t in range(T)])):
                p_in[lb, i] = block.astype(BF16)
            for i in range(T):
                remote(*relay_copy(lb, i)).start()
            update(lb)

        @pl.loop(jnp.maximum(g_here - NEAR + 1, 0), g_here - 1)
        def _(lb):
            for i in range(T):
                arrived(p_in.at[lb, i], pc_r.at[g_here - lb - 1, i])
            update(lb)

        @pl.when(g_here > 0)
        def _():
            wait_m(last)

        found, inner = [], []
        for t in range(T):
            @pl.when(g_here > 0)
            def _(t=t):
                arrived(p_in.at[last, t], pc_r.at[0, t])

            x = acc[t, :, now] - nn(p_in[last, t], m_in[t, last, :, now])
            for s in range(t):
                x = x - nn(inner[s], m_own[s, t, :, now])
            found.append(x)
            inner.append(x[:, :L].astype(BF16))

        @pl.when(g_here < NG - 1)
        def _():
            for i, block in enumerate(across([x[:, L:] for x in found])):
                p_out[g_here + 1, i] = block.astype(BF16)
                remote(*p_chain_copy(g_here + 1, i)).start()

        for i, block in enumerate(across([x[:, :L] for x in found])):
            if i > 0:
                p_out[g_here, i] = jnp.where(quarter < i, block, 0.0).astype(BF16)
                remote(*p_row_copy(g_here, i)).start()

        @pl.when(g_here < NG - 1)
        def _():
            for i in range(T):
                remote(*p_row_copy(g_here + 1, i)).start()

        for ahead in range(2, NEAR):
            @pl.when(g_here < NG - ahead)
            def _(ahead=ahead):
                cols = lanes_of(g_here + ahead, 1)
                later = []
                for t in range(T):
                    x = acc[t, :, cols] - nn(p_in[last, t], m_in[t, last, :, cols])
                    for s in range(t):
                        x = x - nn(inner[s], m_own[s, t, :, cols])
                    later.append(x)
                for i, block in enumerate(across(later)):
                    p_out[g_here + ahead, i] = block.astype(BF16)
                    remote(*p_chain_copy(g_here + ahead, i)).start()
                for i in range(T):
                    remote(*p_row_copy(g_here + ahead, i)).start()

    @pl.when(is_row)
    def _():
        join_z()

        blocks = g_row + jnp.where(t_row > 0, 1, 0)

        def send_slabs(h):
            for far in (g_row + NEAR + 2 * h, g_row + NEAR + 2 * h + 1):
                @pl.when(far < NG)
                def _(far=far):
                    s_out[far] = g_out[:, lanes_of(far, 1)].astype(BF16)
                    remote(*slab_copy(far)).start()

        def term(g):
            arrived(p_row.at[g], pr_r.at[g])
            p = p_row[g]

            @pl.loop(0, (NG - NEAR + 1 - g_row) // 2)
            def _(h):
                cols = lanes_of(g_row + NEAR + 2 * h, 2)
                g_out[:, cols] = g_out[:, cols] - nn(p, m_out[g, :, cols])

                @pl.when(g == blocks - 1)
                def _():
                    send_slabs(h)

            return nn(p, w[g])

        @pl.when(blocks == 0)
        def _():
            pl.loop(0, (NG - NEAR + 1 - g_row) // 2)(send_slabs)

        correction = lax.fori_loop(0, blocks, lambda g, total: total + term(g), jnp.zeros((R, B), F32))
        c_out[...] = correction.astype(BF16)
        for step in (3, 4, 1, 2, 5, 6, 7, 0):
            send(*c_copy((q + step) % N_COL))

    @pl.when(jnp.logical_not(is_row))
    def _():
        join_z()

    pltpu.make_async_copy(z_full, z_out, out_s.at[0]).wait()
    for a in range(2):
        arrived(c_in.at[a], c_r.at[a])

    first_wave(sent)
    each_u(sent, 0)
    second_wave(sent)
    each_v(sent, False, range(BC))
    arrived(zf.at[pl.ds(0, N_COL - 1)], zf_s.at[0])

    @pl.when(is_row)
    def _():
        by_need(lambda lanes: remote(*g_copy(lanes)).wait_send())

        @pl.loop(0, g_row)
        def _(lb):
            by_need(lambda lanes: remote(*m_copy(lb, lanes)).wait_send())

        @pl.loop(0, t_row)
        def _(s):
            by_need(lambda lanes: remote(*own_copy(s, lanes)).wait_send())

        @pl.loop(g_row + NEAR, NG)
        def _(far):
            remote(*slab_copy(far)).wait_send()

        arrived(p_out.at[pl.ds(0, N_COL - 1)], c_s.at[0])

    @pl.when(is_chain)
    def _():
        upto = jnp.minimum(g_here + NEAR, NG)

        arrived(p_out.at[g_here, pl.ds(1, T - 1)], pr_s.at[g_here])

        @pl.loop(g_here + 1, upto)
        def _(g):
            arrived(p_out.at[g], pr_s.at[g])
            arrived(p_out.at[g], pc_s.at[g])

        @pl.loop(0, g_here - NEAR + 1)
        def _(lb):
            arrived(p_in.at[lb], relay_s.at[lb])


def on_device(rhs, inverse_t, u_factors, v_factors, tile_ranks):
    hbm = pl.BlockSpec(memory_space=pl.ANY)
    dma = pltpu.SemaphoreType.DMA
    z, c = pl.pallas_call(
        kernel,
        out_shape=(jax.ShapeDtypeStruct((2, R, B), F32), jax.ShapeDtypeStruct((2, R, B), BF16)),
        in_specs=[pl.BlockSpec(memory_space=pltpu.SMEM), hbm, hbm, hbm, hbm],
        out_specs=(hbm, hbm),
        scratch_shapes=[
            pltpu.VMEM((2, R, B), F32),
            pltpu.VMEM((2, R, B), F32),
            pltpu.VMEM((2, BC, K, B), BF16),
            pltpu.VMEM((2, BC, K, B), BF16),
            pltpu.VMEM((2, BC, K, B), BF16),
            pltpu.VMEM((2, R, B), BF16),
            pltpu.VMEM((R, 2 * R), F32),
            pltpu.VMEM((2, R, 2 * R), BF16),
            pltpu.VMEM((N_COL, R, 2 * R), F32),
            pltpu.VMEM((B, B), BF16),
            pltpu.VMEM((NB, K, B), BF16),
            pltpu.VMEM((NB + (NEAR - 1) * T, K, B), BF16),
            pltpu.VMEM((N_COL, R, 2 * R), BF16),
            pltpu.VMEM((NG, L, B), BF16),
            pltpu.VMEM((NG, L, WIDE), BF16),
            pltpu.VMEM((R, WIDE), F32),
            pltpu.VMEM((NG, R, L), BF16),
            pltpu.VMEM((NG, R, L), BF16),
            pltpu.VMEM((R, B), BF16),
            pltpu.VMEM((2, R, B), F32),
            pltpu.VMEM((T, NG, L, WIDE), BF16),
            pltpu.VMEM((T, T, L, WIDE), BF16),
            pltpu.VMEM((T, R, WIDE), F32),
            pltpu.VMEM((NG, T, R, L), BF16),
            pltpu.VMEM((NG, T, R, L), BF16),
            pltpu.VMEM((NG, T, R, L), BF16),
            dma((4,)), dma((1,)), dma((2,)), dma((2, BC)), dma((2, BC)), dma((2,)), dma((1,)),
            dma((NG,)), dma((T,)), dma((1,)), dma((NG,)), dma((NG,)), dma((NG,)), dma((NG,)), dma((1,)),
            dma((1,)), dma((NG,)), dma((NG,)), dma((1,)), dma((1,)),
            dma((2, NG)), dma((2,)), dma((2,)), dma((NG,)), dma((2, T)), dma((NG,)), dma((2,)),
        ],
        compiler_params=pltpu.CompilerParams(has_side_effects=True, collective_id=0),
    )(
        tile_ranks[:, 0, :, 0], rhs[:, 0], jnp.swapaxes(inverse_t[:, 0], 1, 2),
        u_factors[:, 0, :, 0], v_factors[:, 0, :, 0],
    )
    return (z - c.astype(F32))[:, None]


def solution(mesh):
    in_specs = (
        P(None, "row", None, None),
        P(None, "row", None, "col"),
        P(None, "row", None, "col", None, None),
        P(None, "row", None, "col", None, None),
        P(None, "row", None, "col"),
    )
    out_specs = P(None, "row", None, None)
    return jax.shard_map(
        on_device, mesh=mesh, in_specs=in_specs, out_specs=out_specs, check_vma=False
    )
```

```python
import jax
import jax.numpy as jnp
from jax import lax
from jax.experimental import pallas as pl
from jax.experimental.pallas import tpu as pltpu
from jax.sharding import PartitionSpec as P

B = 512
R = 64
K = 32
BC = 4
N_ROW = 16
N_COL = 8
NB = 32
T = 4
NG = NB // T
L = T * K
NEAR = 3
WIDE = L * (NG + NEAR - 1)
F32 = jnp.float32
BF16 = jnp.bfloat16
MESH = pl.DeviceIdType.MESH


def nn(a, b):
    return jnp.dot(a, b, preferred_element_type=F32)


def nt(a, b, precision=None):
    return lax.dot_general(a, b, (((1,), (1,)), ((), ())), precision=precision, preferred_element_type=F32)


def row_place(j):
    x = ((j % 8) // 2 + 2 * (j // N_ROW)) % 4
    return j % N_ROW, 2 * x + 1


def chain_place(g):
    late = g // 4
    row = ((g + 0 * late) % 4) * 4 + 1 + 1 * late
    return row, 2 * (1 + 1 * late) + 1


def kernel(
    ranks, rhs_hbm, inv_hbm, u_hbm, v_hbm, z_out, c_in,
    rhs, inv, u, v, um, invt, zp, zpb, zf,
    inv_all, u_all, v_all, z_all, w, m_out, g_out, p_row, s_out, c_out, z_full,
    m_in, m_own, acc, s_in, p_in, p_out,
    in_s, out_s, inv_s, u_s, v_s, zb_s, zf_s, m_s, own_s, g_s, s_s, pc_s, c_s,
    inv_r, u_r, v_r, zb_r, zf_r, m_r, own_r, g_r, pc_r, pr_r, c_r,
):
    r = lax.axis_index("row")
    q = lax.axis_index("col")

    q_odd = q % 2 == 1
    x_here = q // 2
    late_row = jnp.where((x_here - (r % 8) // 2) % 4 == 2, 1, 0)
    j_here = r + N_ROW * late_row
    is_row = q_odd & ((x_here - (r % 8) // 2) % 2 == 0)
    g_row = j_here // T
    t_row = j_here % T
    z_here = r % 4
    late_chain = jnp.where((z_here == 2) & (x_here == 2), 1, 0)
    g_here = (r // 4 + 0 * late_chain) % 4 + 4 * late_chain
    is_chain = q_odd & (((z_here == 1) & (x_here == 1)) | (late_chain == 1))

    def is_me(row, col):
        return (row == r) & (col == q)

    def remote(src, dst, ssem, rsem, row, col):
        return pltpu.make_async_remote_copy(
            src_ref=src, dst_ref=dst, send_sem=ssem, recv_sem=rsem,
            device_id=(row, col), device_id_type=MESH,
        )

    def send(src, dst, ssem, rsem, row, col):
        me = is_me(row, col)

        @pl.when(me)
        def _():
            pltpu.make_async_copy(src, dst, rsem).start()

        @pl.when(jnp.logical_not(me))
        def _():
            remote(src, dst, ssem, rsem, row, col).start()

    def sent(src, dst, ssem, rsem, row, col):
        @pl.when(jnp.logical_not(is_me(row, col)))
        def _():
            remote(src, dst, ssem, rsem, row, col).wait_send()

    def arrived(dst, rsem):
        pltpu.make_async_copy(dst, dst, rsem).wait()

    barrier = pltpu.get_barrier_semaphore()

    def greet(row, col):
        @pl.when(jnp.logical_not(is_me(row, col)))
        def _():
            pl.semaphore_signal(barrier, inc=1, device_id=(row, col), device_id_type=MESH)

    for step in range(1, N_COL):
        greet(r, (q + step) % N_COL)

    @pl.when(is_row)
    def _():
        @pl.loop(0, N_ROW)
        def _(row):
            greet(row, j_here % N_COL)

        @pl.loop(jnp.maximum(g_row - NEAR + 1, 0), g_row + 1)
        def _(g):
            greet(*chain_place(g))

    @pl.when(is_chain)
    def _():
        for t in range(T):
            greet(*row_place(g_here * T + t))

        @pl.loop(jnp.maximum(g_here - NEAR + 1, 0), g_here)
        def _(g):
            greet(*chain_place(g))

        @pl.loop(0, T * (g_here - NEAR + 1))
        def _(j):
            greet(*row_place(j))

    expected = N_COL - 1
    for c in range(BC):
        expected += jnp.where(is_me(*row_place(8 * c + q)), 0, 1)
    expected += jnp.where(is_row, 1 + jnp.maximum(NG - NEAR - g_row, 0), 0)
    after = jnp.minimum(NEAR - 1, NG - 1 - g_here)
    expected += jnp.where(is_chain, after + T * (after + 1), 0)

    def inv_copy(a):
        return (
            invt.at[a], inv_all.at[pl.ds(pl.multiple_of(q * R, R), R)],
            inv_s.at[a], inv_r.at[0], *row_place(N_ROW * a + r),
        )

    def u_copy(a, c):
        return (um.at[a, c], u_all.at[8 * c + q], u_s.at[a, c], u_r.at[(8 * c + q) // T], *row_place(N_ROW * a + r))

    def v_copy(a, c):
        return (v.at[a, c], v_all.at[N_ROW * a + r], v_s.at[a, c], v_r.at[(N_ROW * a + r) // T], *row_place(8 * c + q))

    def below(a, c):
        return 8 * c + q < N_ROW * a + r

    def zb_copy(a):
        return (zpb.at[a], z_all.at[q], zb_s.at[a], zb_r.at[0], *row_place(N_ROW * a + r))

    def zf_copy(step):
        return (zp, zf.at[q], zf_s.at[0], zf_r.at[0], r, (q + step) % N_COL)

    loads = [
        pltpu.make_async_copy(src, dst, in_s.at[k])
        for k, (src, dst) in enumerate([(inv_hbm, inv), (rhs_hbm, rhs), (v_hbm, v), (u_hbm, u)])
    ]
    for load in loads:
        load.start()
    loads[0].wait()
    invt[...] = inv[...].astype(BF16)
    loads[1].wait()
    z_mine = [nt(rhs[a], inv[a], lax.Precision.HIGHEST) for a in range(2)]
    zp[...] = jnp.concatenate(z_mine, axis=1)
    for a in range(2):
        wide = jnp.concatenate([z_mine[a], z_mine[a]], axis=1)
        keep = lax.broadcasted_iota(jnp.int32, (R, 2 * R), 1) // R == q % 2
        zpb[a] = jnp.where(keep, wide, 0.0).astype(BF16)

    pl.semaphore_wait(barrier, expected)

    def near(a, c):
        return (N_ROW * a + r) // T - (8 * c + q) // T < NEAR

    def each_v(do, wanted, columns):
        for c in columns:
            for a in range(2):
                @pl.when(below(a, c) & (near(a, c) == wanted))
                def _(a=a, c=c):
                    do(*v_copy(a, c))

    def each_u(do, a):
        for c in range(BC):
            @pl.when(below(a, c))
            def _(c=c):
                do(*u_copy(a, c))

    def first_wave(do):
        do(*zb_copy(0))
        do(*zb_copy(1))
        do(*inv_copy(0))
        each_v(do, True, (0, 1))

    def second_wave(do):
        each_v(do, True, (2, 3))
        do(*inv_copy(1))
        each_u(do, 1)

    def mask_u(a):
        rank_rows = lax.broadcasted_iota(jnp.int32, (K, B), 0)
        for c in range(BC):
            um[a, c] = jnp.where(rank_rows < ranks[a, c], u[a, c].astype(F32), 0.0).astype(BF16)

    loads[2].wait()
    first_wave(send)
    loads[3].wait()
    mask_u(0)
    each_u(send, 0)
    mask_u(1)
    each_v(send, False, (0,))
    second_wave(send)
    each_v(send, False, (1, 2, 3))
    for step in range(N_COL):
        send(*zf_copy(step))

    def lanes_of(g, count):
        return pl.ds(pl.multiple_of(g * L, L), count * L)

    def by_width(g, do):
        for count in range(1, NEAR + 1):
            @pl.when(jnp.minimum(NEAR, NG - g) == count)
            def _(count=count):
                do(count)

    def by_need(do):
        def of(count):
            @pl.when(t_row < T - 1)
            def _():
                do(lanes_of(g_row, count))

            if count > 1:
                @pl.when(t_row == T - 1)
                def _():
                    do(lanes_of(g_row + 1, count - 1))

        by_width(g_row, of)

    half = jnp.where(t_row == T - 1, 1, 0)

    def m_copy(lb, lanes):
        return (
            m_out.at[lb, :, lanes], m_in.at[t_row, lb, :, lanes],
            m_s.at[lb], m_r.at[half, lb], *chain_place(g_row),
        )

    def own_copy(s, lanes):
        return (
            m_out.at[g_row, pl.ds(s * K, K), lanes],
            m_own.at[s, t_row, pl.ds(pl.multiple_of(t_row * K, K), K), lanes],
            own_s.at[s], own_r.at[half], *chain_place(g_row),
        )

    def g_copy(lanes):
        return (
            g_out.at[:, lanes], acc.at[t_row, :, lanes],
            g_s.at[0], g_r.at[half], *chain_place(g_row),
        )

    def slab_copy(g):
        return (s_out.at[g], s_in.at[g_row, t_row], s_s.at[g], u_r.at[g_row], *chain_place(g))

    def c_copy(col):
        return (c_out, c_in.at[j_here // N_ROW], c_s.at[0], c_r.at[j_here // N_ROW], r, col)

    @pl.when(is_row)
    def _():
        here = lanes_of(g_row, NEAR)
        rows = lax.broadcasted_iota(jnp.int32, (L, 1), 0) // K

        @pl.loop(g_row * T, j_here + 1)
        def _(i):
            v_all[i] = jnp.zeros((K, B), BF16)

        arrived(z_all, zb_r.at[0])

        for t in range(T - 1):
            @pl.when(t_row == t)
            def _(t=t):
                arrived(v_all.at[pl.ds(j_here + 1, T - 1 - t)], v_r.at[g_row])

        @pl.loop(g_row + 1, jnp.minimum(g_row + NEAR, NG))
        def _(g):
            arrived(v_all.at[pl.ds(g * T, T)], v_r.at[g])

        def z():
            return jnp.concatenate([z_all[2 * h] + z_all[2 * h + 1] for h in range(N_COL // 2)], axis=1)

        def v_of(g, count):
            return v_all[pl.ds(g * T, count * T)].reshape(count * L, B)

        g_out[:, here] = nt(z(), v_of(g_row, NEAR))
        by_need(lambda lanes: remote(*g_copy(lanes)).start())

        arrived(inv_all, inv_r.at[0])

        def form(lb):
            for count in range(1, T + 1):
                @pl.when(jnp.minimum(T, j_here - lb * T) == count)
                def _(count=count):
                    arrived(u_all.at[pl.ds(lb * T, count)], u_r.at[lb])

            wl = nt(u_all[pl.ds(lb * T, T)].reshape(L, B), inv_all[...])
            wl = jnp.where(rows + lb * T < j_here, wl, 0.0).astype(BF16)
            w[lb] = wl
            m_out[lb, :, here] = nt(wl, v_of(g_row, NEAR)).astype(BF16)

        form(g_row)

        @pl.loop(0, t_row)
        def _(s):
            by_need(lambda lanes: remote(*own_copy(s, lanes)).start())

        @pl.loop(0, g_row)
        def _(lb):
            form(lb)
            by_need(lambda lanes: remote(*m_copy(lb, lanes)).start())

        @pl.loop(g_row + NEAR, NG)
        def _(g):
            arrived(v_all.at[pl.ds(g * T, T)], v_r.at[g])

        @pl.loop(0, (NG - NEAR + 1 - g_row) // 2)
        def _(h):
            far = g_row + NEAR + 2 * h
            cols = lanes_of(far, 2)
            g_out[:, cols] = nt(z(), v_of(far, 2))

            @pl.loop(0, g_row + 1)
            def _(lb):
                m_out[lb, :, cols] = nt(w[lb], v_of(far, 2)).astype(BF16)

    def join_z():
        arrived(zf, zf_r.at[0])
        for a in range(2):
            z_full[a] = jnp.concatenate([zf[col][:, a * R:(a + 1) * R] for col in range(N_COL)], axis=1)
        pltpu.make_async_copy(z_full, z_out, out_s.at[0]).start()

    def p_chain_copy(g, i):
        return (p_out.at[g, i], p_in.at[g_here, i], pc_s.at[g], pc_r.at[g - g_here - 1, i], *chain_place(g))

    def p_row_copy(g, i):
        return (p_out.at[g, i], p_row.at[g_here], m_s.at[g], pr_r.at[g_here], *row_place(g * T + i))

    def relay_copy(lb, i):
        return (p_in.at[lb, i], p_row.at[lb], s_s.at[lb], pr_r.at[lb], *row_place(g_here * T + i))

    @pl.when(is_chain)
    def _():
        quarter = lax.broadcasted_iota(jnp.int32, (R, L), 1) // K
        last = jnp.maximum(g_here - 1, 0)

        def across(parts):
            gives = []
            for i in range(T):
                row = parts[0] if i == 0 else pltpu.roll(parts[0], (L - K * i) % L, 1)
                for t in range(1, T):
                    shift = (K * (t - i)) % L
                    row = jnp.where(quarter == t, parts[t] if shift == 0 else pltpu.roll(parts[t], shift, 1), row)
                gives.append(row)
            return gives

        for s in range(T):
            for t in range(s + 1, T):
                for i in range(T):
                    if i != t:
                        m_own[s, t, i * K:(i + 1) * K, :] = jnp.zeros((K, WIDE), BF16)

        @pl.when(g_here == 0)
        def _():
            p_in[0] = jnp.zeros((T, R, L), BF16)
            for t in range(T):
                m_in[t, 0] = jnp.zeros((L, WIDE), BF16)

        here = lanes_of(g_here, NEAR)
        now = lanes_of(g_here, 2)

        def wait_m(lb):
            def of(count):
                arrived(m_in.at[pl.ds(0, T - 1), lb, :, lanes_of(g_here, count)], m_r.at[0, lb])
                if count > 1:
                    arrived(m_in.at[T - 1, lb, :, lanes_of(g_here + 1, count - 1)], m_r.at[1, lb])

            by_width(g_here, of)

        def update(lb):
            wait_m(lb)
            for t in range(T):
                acc[t, :, here] = acc[t, :, here] - nn(p_in[lb, t], m_in[t, lb, :, here])

        def wait_start(count):
            lanes = lanes_of(g_here, count)
            arrived(acc.at[pl.ds(0, T - 1), :, lanes], g_r.at[0])
            arrived(m_own.at[0, 0, pl.ds(0, 3 * K), lanes], own_r.at[0])
            if count > 1:
                lanes = lanes_of(g_here + 1, count - 1)
                arrived(acc.at[T - 1, :, lanes], g_r.at[1])
                arrived(m_own.at[0, 0, pl.ds(0, 3 * K), lanes], own_r.at[1])

        by_width(g_here, wait_start)

        @pl.loop(0, g_here - NEAR + 1)
        def _(lb):
            arrived(s_in.at[lb], u_r.at[lb])
            for i, block in enumerate(across([s_in[lb, t].astype(F32) for t in range(T)])):
                p_in[lb, i] = block.astype(BF16)
            for i in range(T):
                remote(*relay_copy(lb, i)).start()
            update(lb)

        @pl.loop(jnp.maximum(g_here - NEAR + 1, 0), g_here - 1)
        def _(lb):
            for i in range(T):
                arrived(p_in.at[lb, i], pc_r.at[g_here - lb - 1, i])
            update(lb)

        @pl.when(g_here > 0)
        def _():
            wait_m(last)

        found, inner = [], []
        for t in range(T):
            @pl.when(g_here > 0)
            def _(t=t):
                arrived(p_in.at[last, t], pc_r.at[0, t])

            x = acc[t, :, now] - nn(p_in[last, t], m_in[t, last, :, now])
            for s in range(t):
                x = x - nn(inner[s], m_own[s, t, :, now])
            found.append(x)
            inner.append(x[:, :L].astype(BF16))

        @pl.when(g_here < NG - 1)
        def _():
            for i, block in enumerate(across([x[:, L:] for x in found])):
                p_out[g_here + 1, i] = block.astype(BF16)
                remote(*p_chain_copy(g_here + 1, i)).start()

        for i, block in enumerate(across([x[:, :L] for x in found])):
            if i > 0:
                p_out[g_here, i] = jnp.where(quarter < i, block, 0.0).astype(BF16)
                remote(*p_row_copy(g_here, i)).start()

        @pl.when(g_here < NG - 1)
        def _():
            for i in range(T):
                remote(*p_row_copy(g_here + 1, i)).start()

        for ahead in range(2, NEAR):
            @pl.when(g_here < NG - ahead)
            def _(ahead=ahead):
                cols = lanes_of(g_here + ahead, 1)
                later = []
                for t in range(T):
                    x = acc[t, :, cols] - nn(p_in[last, t], m_in[t, last, :, cols])
                    for s in range(t):
                        x = x - nn(inner[s], m_own[s, t, :, cols])
                    later.append(x)
                for i, block in enumerate(across(later)):
                    p_out[g_here + ahead, i] = block.astype(BF16)
                    remote(*p_chain_copy(g_here + ahead, i)).start()
                for i in range(T):
                    remote(*p_row_copy(g_here + ahead, i)).start()

    @pl.when(is_row)
    def _():
        join_z()

        blocks = g_row + jnp.where(t_row > 0, 1, 0)

        def send_slabs(h):
            for far in (g_row + NEAR + 2 * h, g_row + NEAR + 2 * h + 1):
                @pl.when(far < NG)
                def _(far=far):
                    s_out[far] = g_out[:, lanes_of(far, 1)].astype(BF16)
                    remote(*slab_copy(far)).start()

        def term(g):
            arrived(p_row.at[g], pr_r.at[g])
            p = p_row[g]

            @pl.loop(0, (NG - NEAR + 1 - g_row) // 2)
            def _(h):
                cols = lanes_of(g_row + NEAR + 2 * h, 2)
                g_out[:, cols] = g_out[:, cols] - nn(p, m_out[g, :, cols])

                @pl.when(g == blocks - 1)
                def _():
                    send_slabs(h)

            return nn(p, w[g])

        @pl.when(blocks == 0)
        def _():
            pl.loop(0, (NG - NEAR + 1 - g_row) // 2)(send_slabs)

        correction = lax.fori_loop(0, blocks, lambda g, total: total + term(g), jnp.zeros((R, B), F32))
        c_out[...] = correction.astype(BF16)
        for step in (3, 4, 1, 2, 5, 6, 7, 0):
            send(*c_copy((q + step) % N_COL))

    @pl.when(jnp.logical_not(is_row))
    def _():
        join_z()

    pltpu.make_async_copy(z_full, z_out, out_s.at[0]).wait()
    for a in range(2):
        arrived(c_in.at[a], c_r.at[a])

    first_wave(sent)
    each_u(sent, 0)
    second_wave(sent)
    each_v(sent, False, range(BC))
    arrived(zf.at[pl.ds(0, N_COL - 1)], zf_s.at[0])

    @pl.when(is_row)
    def _():
        by_need(lambda lanes: remote(*g_copy(lanes)).wait_send())

        @pl.loop(0, g_row)
        def _(lb):
            by_need(lambda lanes: remote(*m_copy(lb, lanes)).wait_send())

        @pl.loop(0, t_row)
        def _(s):
            by_need(lambda lanes: remote(*own_copy(s, lanes)).wait_send())

        @pl.loop(g_row + NEAR, NG)
        def _(far):
            remote(*slab_copy(far)).wait_send()

        arrived(p_out.at[pl.ds(0, N_COL - 1)], c_s.at[0])

    @pl.when(is_chain)
    def _():
        upto = jnp.minimum(g_here + NEAR, NG)

        arrived(p_out.at[g_here, pl.ds(1, T - 1)], m_s.at[g_here])

        @pl.loop(g_here + 1, upto)
        def _(g):
            arrived(p_out.at[g], m_s.at[g])
            arrived(p_out.at[g], pc_s.at[g])

        @pl.loop(0, g_here - NEAR + 1)
        def _(lb):
            arrived(p_in.at[lb], s_s.at[lb])


def on_device(rhs, inverse_t, u_factors, v_factors, tile_ranks):
    hbm = pl.BlockSpec(memory_space=pl.ANY)
    dma = pltpu.SemaphoreType.DMA
    z, c = pl.pallas_call(
        kernel,
        out_shape=(jax.ShapeDtypeStruct((2, R, B), F32), jax.ShapeDtypeStruct((2, R, B), BF16)),
        in_specs=[pl.BlockSpec(memory_space=pltpu.SMEM), hbm, hbm, hbm, hbm],
        out_specs=(hbm, hbm),
        scratch_shapes=[
            pltpu.VMEM((2, R, B), F32),
            pltpu.VMEM((2, R, B), F32),
            pltpu.VMEM((2, BC, K, B), BF16),
            pltpu.VMEM((2, BC, K, B), BF16),
            pltpu.VMEM((2, BC, K, B), BF16),
            pltpu.VMEM((2, R, B), BF16),
            pltpu.VMEM((R, 2 * R), F32),
            pltpu.VMEM((2, R, 2 * R), BF16),
            pltpu.VMEM((N_COL, R, 2 * R), F32),
            pltpu.VMEM((B, B), BF16),
            pltpu.VMEM((NB, K, B), BF16),
            pltpu.VMEM((NB + (NEAR - 1) * T, K, B), BF16),
            pltpu.VMEM((N_COL, R, 2 * R), BF16),
            pltpu.VMEM((NG, L, B), BF16),
            pltpu.VMEM((NG, L, WIDE), BF16),
            pltpu.VMEM((R, WIDE), F32),
            pltpu.VMEM((NG, R, L), BF16),
            pltpu.VMEM((NG, R, L), BF16),
            pltpu.VMEM((R, B), BF16),
            pltpu.VMEM((2, R, B), F32),
            pltpu.VMEM((T, NG, L, WIDE), BF16),
            pltpu.VMEM((T, T, L, WIDE), BF16),
            pltpu.VMEM((T, R, WIDE), F32),
            pltpu.VMEM((NG, T, R, L), BF16),
            pltpu.VMEM((NG, T, R, L), BF16),
            pltpu.VMEM((NG, T, R, L), BF16),
            dma((4,)), dma((1,)), dma((2,)), dma((2, BC)), dma((2, BC)), dma((2,)), dma((1,)),
            dma((NG,)), dma((T,)), dma((1,)), dma((NG,)), dma((NG,)), dma((1,)),
            dma((1,)), dma((NG,)), dma((NG,)), dma((1,)), dma((1,)),
            dma((2, NG)), dma((2,)), dma((2,)), dma((2, T)), dma((NG,)), dma((2,)),
        ],
        compiler_params=pltpu.CompilerParams(has_side_effects=True, collective_id=0),
    )(
        tile_ranks[:, 0, :, 0], rhs[:, 0], jnp.swapaxes(inverse_t[:, 0], 1, 2),
        u_factors[:, 0, :, 0], v_factors[:, 0, :, 0],
    )
    return (z - c.astype(F32))[:, None]


def solution(mesh):
    in_specs = (
        P(None, "row", None, None),
        P(None, "row", None, "col"),
        P(None, "row", None, "col", None, None),
        P(None, "row", None, "col", None, None),
        P(None, "row", None, "col"),
    )
    out_specs = P(None, "row", None, None)
    return jax.shard_map(
        on_device, mesh=mesh, in_specs=in_specs, out_specs=out_specs, check_vma=False
    )
```
